8 devices in a mesh: data: 1 (over z), ctxo: 2 (over y), ctx: 4 (over x, core).
Axes of the slice: x: 2, y: 2, z: 1, core: 2. Of those that a mesh axis runs over, the one named last changes fastest.
Arguments:
- q_seq: bfloat16 [16, 4096, 4, 128], P('data', ('ctxo', 'ctx'))
- k_seq: bfloat16 [16, 4096, 1, 128], P('data', ('ctxo', 'ctx'))
- v_seq: bfloat16 [16, 4096, 1, 128], P('data', ('ctxo', 'ctx'))
- do_seq: bfloat16 [16, 4096, 4, 128], P('data', ('ctxo', 'ctx'))
Outputs:
- output 1: bfloat16 [16, 4096, 4, 128], P('data', ('ctxo', 'ctx'))
- output 2: bfloat16 [16, 4096, 4, 128], P('data', ('ctxo', 'ctx'))
- output 3: bfloat16 [16, 4096, 1, 128], P('data', ('ctxo', 'ctx'))
- output 4: bfloat16 [16, 4096, 1, 128], P('data', ('ctxo', 'ctx'))
All inputs are finite; a program needn't handle non-finite values.
Results may differ from the reference program's by a relative error of at most 0.0124163.
Values are sent between devices in bfloat16 or wider.
A program may use at most 1 GiB of HBM per device.

```python
import math
import jax
import jax.numpy as jnp
from jax import lax

BATCH_SEQS = 16
SEQ_LEN = 4096
Q_LOCAL = 4
KV_LOCAL = 1
HEAD_DIM = 128
ROW_BLOCK = 64


def setup_inputs(seed: int = 0, part: int = 0) -> dict:
    base_key = jax.random.fold_in(jax.random.key(seed), part)
    key_q, key_k, key_v, key_d = jax.random.split(base_key, 4)
    q_shape = (BATCH_SEQS, SEQ_LEN, Q_LOCAL, HEAD_DIM)
    kv_shape = (BATCH_SEQS, SEQ_LEN, KV_LOCAL, HEAD_DIM)
    spread = math.sqrt(1.0 + math.log(max(SEQ_LEN / 256.0, 1.0)))
    q_seq = spread * jax.random.normal(key_q, q_shape, jnp.float32)
    k_seq = jax.random.normal(key_k, kv_shape, jnp.float32)
    v_seq = jax.random.normal(key_v, kv_shape, jnp.float32)
    do_seq = jax.random.normal(key_d, q_shape, jnp.float32)
    return {'q_seq': q_seq.astype(jnp.bfloat16), 'k_seq': k_seq.astype(jnp.bfloat16), 'v_seq': v_seq.astype(jnp.bfloat16), 'do_seq': do_seq.astype(jnp.bfloat16)}


def reference(q_seq, k_seq, v_seq, do_seq):
    group_size = Q_LOCAL // KV_LOCAL
    n_blocks = SEQ_LEN // ROW_BLOCK
    q_scale = 1.0 / math.sqrt(HEAD_DIM)
    blocked = (BATCH_SEQS, n_blocks, ROW_BLOCK, KV_LOCAL, group_size, HEAD_DIM)
    q_rows = jnp.moveaxis(q_seq.astype(jnp.float32).reshape(blocked), 1, 0)
    do_rows = jnp.moveaxis(do_seq.astype(jnp.float32).reshape(blocked), 1, 0)
    key_pos = lax.broadcasted_iota(jnp.int32, (1, 1, SEQ_LEN), 2)
    row_pos = lax.broadcasted_iota(jnp.int32, (ROW_BLOCK, 1, 1), 0)

    def attention(q_blocks, keys_all, vals_all):
        def one_block(block_in):
            q_blk, blk_idx = block_in
            scores = jnp.einsum('bqhgd,bkhd->bhqgk', q_blk, keys_all) * q_scale
            visible = row_pos + blk_idx * ROW_BLOCK >= key_pos
            probs_blk = jax.nn.softmax(jnp.where(visible, scores, -jnp.inf), axis=-1)
            return jnp.einsum('bhqgk,bkhd->bqhgd', probs_blk, vals_all)
        return lax.map(jax.checkpoint(one_block), (q_blocks, jnp.arange(n_blocks)))

    out_rows, pull_back = jax.vjp(attention, q_rows, k_seq.astype(jnp.float32), v_seq.astype(jnp.float32))
    dq_rows, dk_all, dv_all = pull_back(do_rows)
    q_full = (BATCH_SEQS, SEQ_LEN, Q_LOCAL, HEAD_DIM)
    out_seq = jnp.moveaxis(out_rows, 0, 1).reshape(q_full)
    dq_seq = jnp.moveaxis(dq_rows, 0, 1).reshape(q_full)
    return (out_seq.astype(jnp.bfloat16), dq_seq.astype(jnp.bfloat16), dk_all.astype(jnp.bfloat16), dv_all.astype(jnp.bfloat16))
```

```python
import functools
import math

import jax
import jax.numpy as jnp
from jax import lax
from jax.experimental import pallas as pl
from jax.experimental.pallas import tpu as pltpu
from jax.sharding import PartitionSpec as P

MESH = pl.DeviceIdType.MESH
NT = (((1,), (1,)), ((), ()))
F32 = jnp.float32
BF16 = jnp.bfloat16
NDEV = 8
BLK = 512
QR = 4 * BLK
HD = 128
SEQ = NDEV * BLK
SCALE = 1.0 / math.sqrt(HD)
SCALE2 = SCALE * math.log2(math.e)
DIAG = 256
RA = 1024
RB = 1024
RC = 1024
NSLOT = 4


def lane_fold(op, s):
    acc = s[:, 0:128]
    for g in range(1, s.shape[1] // 128):
        acc = op(acc, s[:, g * 128:(g + 1) * 128])
    return acc


def lanes(x, width):
    return jnp.tile(x, (1, width // 128))


def attn_tile(blk, slot, oslot, kv, qb, dob, kb, vb, ob, dqb, S, dkt, dvt, oacc, dqacc, mx, lx, qT, doT, after_forward, before_pass_c):
    own = pl.multiple_of(blk * BLK, BLK)
    blocks = lambda n: [(r, n) for r in range(0, QR, n)]

    def diag(fn):
        for u in reversed(range(BLK // DIAG)):
            fn(u, DIAG * (u + 1), u * DIAG * 4, DIAG * 4)

    def score_diag(u, w, r, n):
        rs = pl.ds(r, n)
        s = lax.dot_general(qb[slot, rs, :], kb[kv, pl.ds(own, w), :], NT, preferred_element_type=F32)
        row = lax.broadcasted_iota(jnp.int32, (n, DIAG), 0) // 4
        col = lax.broadcasted_iota(jnp.int32, (n, DIAG), 1)
        sd = jnp.where(row >= col, s[:, w - DIAG:], -1e30)
        S[rs, pl.ds(own + (w - DIAG), DIAG)] = sd
        m = lane_fold(jnp.maximum, sd)
        if w > DIAG:
            S[rs, pl.ds(own, w - DIAG)] = s[:, :w - DIAG]
            m = jnp.maximum(m, lane_fold(jnp.maximum, s[:, :w - DIAG]))
        mx[rs, :] = m

    diag(score_diag)
    qT[...] = qb[slot].T
    doT[...] = dob[slot].T

    @pl.loop(0, blk)
    def _(j):
        o = pl.multiple_of(j * BLK, BLK)
        for r, n in blocks(RA):
            rs = pl.ds(r, n)
            s = lax.dot_general(qb[slot, rs, :], kb[kv, pl.ds(o, BLK), :], NT, preferred_element_type=F32)
            S[rs, pl.ds(o, BLK)] = s
            mx[rs, :] = jnp.maximum(mx[rs, :], lane_fold(jnp.maximum, s))

    mx[...] = jnp.broadcast_to(jnp.max(mx[...], axis=1, keepdims=True) * SCALE2, (QR, 128))

    def probs(o, w, r, n, first):
        rs = pl.ds(r, n)
        p = jnp.exp2(S[rs, pl.ds(o, w)] * SCALE2 - lanes(mx[rs, :], w))
        S[rs, pl.ds(o, w)] = p
        ls = lane_fold(jnp.add, p)
        oo = jnp.dot(p.astype(BF16), vb[kv, pl.ds(o, w), :], preferred_element_type=F32)
        if first:
            lx[rs, :] = ls
            oacc[rs, :] = oo
        else:
            lx[rs, :] += ls
            oacc[rs, :] += oo

    diag(lambda u, w, r, n: probs(own, w, r, n, True))

    @pl.loop(0, blk)
    def _(j):
        o = pl.multiple_of(j * BLK, BLK)
        for r, n in blocks(RB):
            probs(o, BLK, r, n, False)

    lx[...] = jnp.broadcast_to(1.0 / jnp.sum(lx[...], axis=1, keepdims=True), (QR, 128))
    out = oacc[...] * lx[...]
    ob[oslot] = out.astype(BF16)
    mx[...] = jnp.broadcast_to(jnp.sum(out * dob[slot].astype(F32), axis=1, keepdims=True), (QR, 128))
    after_forward()
    before_pass_c()

    def grads(o, w, r, n):
        rs = pl.ds(r, n)
        pn = S[rs, pl.ds(o, w)] * lanes(lx[rs, :], w)
        gv = jnp.dot(doT[:, rs], pn.astype(BF16), preferred_element_type=F32)
        dp = lax.dot_general(dob[slot, rs, :], vb[kv, pl.ds(o, w), :], NT, preferred_element_type=F32)
        ds = (pn * (dp - lanes(mx[rs, :], w))).astype(BF16)
        gk = jnp.dot(qT[:, rs], ds, preferred_element_type=F32)
        gq = jnp.dot(ds, kb[kv, pl.ds(o, w), :], preferred_element_type=F32)
        return gv, gk, gq

    def grads_diag(u, w, r, n):
        gv, gk, gq = grads(own, w, r, n)
        dqacc[pl.ds(r, n), :] = gq
        dvt[:, pl.ds(own, w)] += gv
        dkt[:, pl.ds(own, w)] += gk

    diag(grads_diag)

    @pl.loop(0, blk)
    def _(j):
        o = pl.multiple_of(j * BLK, BLK)
        av, ak = None, None
        for r, n in blocks(RC):
            gv, gk, gq = grads(o, BLK, r, n)
            dqacc[pl.ds(r, n), :] += gq
            av = gv if av is None else av + gv
            ak = gk if ak is None else ak + gk
        dvt[:, pl.ds(o, BLK)] += av
        dkt[:, pl.ds(o, BLK)] += ak

    dqb[oslot] = (dqacc[...] * SCALE).astype(BF16)


def kernel(q, do, k, v, out, dq, dk, dv, qr, dor, kr, vr,
           qb, dob, kb, vb, ob, dqb, kst, vst, S, dkt, dvt, oacc, dqacc, mx, lx, qT, doT,
           send, recv, rsend, rrecv, load, lout):
    y = lax.axis_index('ctxo')
    b = lax.axis_index('ctx')
    x = b // 2
    core = lax.rem(b, 2)
    me = y * 4 + b

    def device(d):
        return (0, d // 4, lax.rem(d, 4))

    def partner(step):
        off = lax.rem(2 * step, NDEV) + step // 4
        return (lax.rem(y + off // 4, 2) * 4 + lax.rem(x + lax.rem(off // 2, 2), 2) * 2
                + lax.rem(core + lax.rem(off, 2), 2))

    barrier = pltpu.get_barrier_semaphore()
    for step in range(1, NDEV):
        pl.semaphore_signal(barrier, inc=1, device_id=device(partner(step)), device_id_type=MESH)
    pl.semaphore_wait(barrier, NDEV - 1)

    src = (k, v, q, do)
    dst = (kr, vr, qr, dor)

    def ship(t, rr, step):
        h = partner(step)
        return pltpu.make_async_remote_copy(
            src_ref=src[t].at[2 * h + rr], dst_ref=dst[t].at[rr, me],
            send_sem=send.at[t, rr, step], recv_sem=recv.at[t, rr, me],
            device_id=device(h), device_id_type=MESH)

    def arrival(t, rr, i):
        return pltpu.make_async_remote_copy(
            src_ref=src[t].at[0], dst_ref=dst[t].at[rr, i],
            send_sem=send.at[t, rr, 0], recv_sem=recv.at[t, rr, i],
            device_id=device(partner(1)), device_id_type=MESH)

    @pl.loop(1, NDEV)
    def _(step):
        ship(0, 0, step).start()
        ship(1, 0, step).start()

    @pl.loop(1, NDEV)
    def _(step):
        ship(2, 0, step).start()
        ship(3, 0, step).start()

    bufs = (kb, vb, qb, dob)

    def kv_copies(rr, i, own):
        o = pl.ds(pl.multiple_of(i * BLK, BLK), BLK)
        for t in range(2):
            source = src[t].at[2 * me + rr] if own else dst[t].at[rr, i]
            yield pltpu.make_async_copy(source, bufs[t].at[rr, o, :], load.at[t, i])

    def fetch_kv(rr):
        for c in kv_copies(rr, me, True):
            c.start()

        @pl.loop(1, NDEV)
        def _(step):
            i = partner(step)
            arrival(0, rr, i).wait_recv()
            arrival(1, rr, i).wait_recv()
            for c in kv_copies(rr, i, False):
                c.start()

        @pl.loop(0, NDEV)
        def _(i):
            for c in kv_copies(rr, i, False):
                c.wait()

    def fetch(rr, step, slot):
        i = partner(step)

        @pl.when(step == 0)
        def _():
            for t in (2, 3):
                pltpu.make_async_copy(src[t].at[2 * me + rr], bufs[t].at[slot], load.at[t, 0]).start()

        @pl.when(step != 0)
        def _():
            for t in (2, 3):
                arrival(t, rr, i).wait_recv()
                pltpu.make_async_copy(dst[t].at[rr, i], bufs[t].at[slot], load.at[t, 0]).start()

    def fetch_wait(rr, step, slot):
        for t in (2, 3):
            pltpu.make_async_copy(dst[t].at[rr, partner(step)], bufs[t].at[slot], load.at[t, 0]).wait()

    rbuf = (ob, dqb, kst, vst)
    rdst = (out, dq, dk, dv)

    def reply(t, task):
        rr = task // NDEV
        i = partner(lax.rem(task, NDEV))
        if t < 2:
            idx = lax.rem(task, NSLOT)
            source = rbuf[t].at[idx]
        else:
            idx = i
            source = rbuf[t].at[pl.ds(pl.multiple_of(i * BLK, BLK), BLK), :]
        row = 2 * me + rr
        remote = pltpu.make_async_remote_copy(
            src_ref=source, dst_ref=rdst[t].at[row],
            send_sem=rsend.at[t, idx], recv_sem=rrecv.at[t, row],
            device_id=device(i), device_id_type=MESH)
        local = pltpu.make_async_copy(source, rdst[t].at[row], lout.at[t])
        return remote, local

    def reply_start(t, task):
        remote, local = reply(t, task)

        @pl.when(lax.rem(task, NDEV) == 0)
        def _():
            local.start()

        @pl.when(lax.rem(task, NDEV) != 0)
        def _():
            remote.start()

    def reply_wait(t, task):
        remote, local = reply(t, task)

        @pl.when(lax.rem(task, NDEV) == 0)
        def _():
            local.wait()

        @pl.when(lax.rem(task, NDEV) != 0)
        def _():
            remote.wait_send()

    fetch(0, 0, 0)

    @pl.loop(0, 2 * NDEV)
    def _(task):
        rr = task // NDEV
        step = lax.rem(task, NDEV)
        i = partner(step)
        slot = lax.rem(task, 2)
        oslot = lax.rem(task, NSLOT)

        @pl.when(step == 0)
        def _():
            fetch_kv(rr)
            dkt[...] = jnp.zeros_like(dkt)
            dvt[...] = jnp.zeros_like(dvt)

        @pl.when(task == 0)
        def _():
            @pl.loop(1, NDEV)
            def _(s):
                ship(0, 1, s).start()
                ship(1, 1, s).start()

        @pl.when((task > 0) & (task < NDEV))
        def _():
            ship(2, 1, step).start()
            ship(3, 1, step).start()

        fetch_wait(rr, step, slot)

        def after_forward():
            reply_start(0, task)

        def before_pass_c():
            @pl.when(task + 1 < 2 * NDEV)
            def _():
                fetch((task + 1) // NDEV, lax.rem(task + 1, NDEV), lax.rem(task + 1, 2))

        @pl.when(task >= NSLOT)
        def _():
            reply_wait(0, task - NSLOT)
            reply_wait(1, task - NSLOT)

        attn_tile(i, slot, oslot, rr, qb, dob, kb, vb, ob, dqb, S, dkt, dvt, oacc, dqacc, mx, lx, qT, doT,
                  after_forward, before_pass_c)
        reply_start(1, task)

        @pl.when(step == NDEV - 1)
        def _():
            @pl.when(rr > 0)
            def _():
                @pl.loop(0, NDEV)
                def _(s):
                    reply_wait(2, s)
                    reply_wait(3, s)

            @pl.loop(0, NDEV)
            def _(s):
                o = pl.multiple_of(partner(s) * BLK, BLK)
                kst[pl.ds(o, BLK), :] = (dkt[:, pl.ds(o, BLK)] * SCALE).T.astype(BF16)
                vst[pl.ds(o, BLK), :] = dvt[:, pl.ds(o, BLK)].T.astype(BF16)
                reply_start(2, rr * NDEV + s)
                reply_start(3, rr * NDEV + s)

    @pl.loop(2 * NDEV - NSLOT, 2 * NDEV)
    def _(task):
        reply_wait(0, task)
        reply_wait(1, task)

    @pl.loop(NDEV, 2 * NDEV)
    def _(task):
        reply_wait(2, task)
        reply_wait(3, task)

    @pl.loop(1, NDEV)
    def _(step):
        for rr in range(2):
            for t in range(4):
                ship(t, rr, step).wait_send()

    @pl.loop(0, 2 * NDEV)
    def _(row):
        @pl.when(row // 2 != me)
        def _():
            for t in range(4):
                source = rbuf[t].at[0] if t < 2 else rbuf[t].at[pl.ds(0, BLK), :]
                pltpu.make_async_remote_copy(
                    src_ref=source, dst_ref=rdst[t].at[row],
                    send_sem=rsend.at[t, 0], recv_sem=rrecv.at[t, row],
                    device_id=device(partner(1)), device_id_type=MESH).wait_recv()


def solution(mesh):
    spec = P('data', ('ctxo', 'ctx'), None, None)
    any_spec = pl.BlockSpec(memory_space=pl.ANY)

    def local_attn(q_in, k_in, v_in, do_in):
        rows = q_in.shape[0]
        wide = jax.ShapeDtypeStruct((rows, QR, HD), BF16)
        narrow = jax.ShapeDtypeStruct((rows, BLK, HD), BF16)
        land_wide = jax.ShapeDtypeStruct((2, NDEV, QR, HD), BF16)
        land_narrow = jax.ShapeDtypeStruct((2, NDEV, BLK, HD), BF16)
        call = pl.pallas_call(
            kernel,
            out_shape=[wide, wide, narrow, narrow, land_wide, land_wide, land_narrow, land_narrow],
            in_specs=[any_spec] * 4,
            out_specs=[any_spec] * 8,
            scratch_shapes=[
                pltpu.VMEM((2, QR, HD), BF16), pltpu.VMEM((2, QR, HD), BF16),
                pltpu.VMEM((2, SEQ, HD), BF16), pltpu.VMEM((2, SEQ, HD), BF16),
                pltpu.VMEM((NSLOT, QR, HD), BF16), pltpu.VMEM((NSLOT, QR, HD), BF16),
                pltpu.VMEM((SEQ, HD), BF16), pltpu.VMEM((SEQ, HD), BF16),
                pltpu.VMEM((QR, SEQ), F32),
                pltpu.VMEM((HD, SEQ), F32), pltpu.VMEM((HD, SEQ), F32),
                pltpu.VMEM((QR, HD), F32), pltpu.VMEM((QR, HD), F32),
                pltpu.VMEM((QR, 128), F32), pltpu.VMEM((QR, 128), F32),
                pltpu.VMEM((HD, QR), BF16), pltpu.VMEM((HD, QR), BF16),
                pltpu.SemaphoreType.DMA((4, 2, NDEV)), pltpu.SemaphoreType.DMA((4, 2, NDEV)),
                pltpu.SemaphoreType.DMA((4, NDEV)), pltpu.SemaphoreType.DMA((4, 2 * NDEV)),
                pltpu.SemaphoreType.DMA((4, NDEV)), pltpu.SemaphoreType.DMA((4,)),
            ],
            compiler_params=pltpu.CompilerParams(
                collective_id=0, has_side_effects=True, vmem_limit_bytes=67043328),
        )
        res = call(q_in.reshape(rows, QR, HD), do_in.reshape(rows, QR, HD),
                   k_in.reshape(rows, BLK, HD), v_in.reshape(rows, BLK, HD))
        return (res[0].reshape(q_in.shape), res[1].reshape(q_in.shape),
                res[2].reshape(k_in.shape), res[3].reshape(v_in.shape))

    return jax.shard_map(local_attn, mesh=mesh, in_specs=(spec,) * 4, out_specs=(spec,) * 4, check_vma=False)
```

```python
import functools
import math

import jax
import jax.numpy as jnp
from jax import lax
from jax.experimental import pallas as pl
from jax.experimental.pallas import tpu as pltpu
from jax.sharding import PartitionSpec as P

MESH = pl.DeviceIdType.MESH
NT = (((1,), (1,)), ((), ()))
F32 = jnp.float32
BF16 = jnp.bfloat16
NDEV = 8
BLK = 512
QR = 4 * BLK
HD = 128
SEQ = NDEV * BLK
SCALE = 1.0 / math.sqrt(HD)
SCALE2 = SCALE * math.log2(math.e)
DIAG = 256
RA = 1024
RB = 1024
RC = 1024
NSLOT = 2
NA = 10
NP = NA // 2
DIRECT = 5
HOMES = (0, 0, 1, 2, 4, 5)
HSLOT = (0, 1, 0, 0, 0, 0)
EARLY = (0, 3, 2)
LATER = ((), (), (), (1,), (4, 5))


def lane_fold(op, s):
    acc = s[:, 0:128]
    for g in range(1, s.shape[1] // 128):
        acc = op(acc, s[:, g * 128:(g + 1) * 128])
    return acc


def lanes(x, width):
    return jnp.tile(x, (1, width // 128))


def attn_tile(blk, slot, oslot, kv, qb, dob, kb, vb, ob, dqb, S, acc, aslot, oacc, mx, lx, qT, doT, after_forward, before_pass_c):
    own = pl.multiple_of(blk * BLK, BLK)
    blocks = lambda n: [(r, n) for r in range(0, QR, n)]

    def diag(fn):
        for u in reversed(range(BLK // DIAG)):
            fn(u, DIAG * (u + 1), u * DIAG * 4, DIAG * 4)

    def sweep(chunk):
        @pl.loop(0, blk // 2)
        def _(j):
            chunk(pl.multiple_of(2 * j * BLK, BLK))
            chunk(pl.multiple_of((2 * j + 1) * BLK, BLK))

        @pl.when(lax.rem(blk, 2) == 1)
        def _():
            chunk(pl.multiple_of((blk - 1) * BLK, BLK))

    def score_diag(u, w, r, n):
        rs = pl.ds(r, n)
        s = lax.dot_general(qb[slot, rs, :], kb[kv, pl.ds(own, w), :], NT, preferred_element_type=F32)
        row = lax.broadcasted_iota(jnp.int32, (n, DIAG), 0) // 4
        col = lax.broadcasted_iota(jnp.int32, (n, DIAG), 1)
        sd = jnp.where(row >= col, s[:, w - DIAG:], -1e30)
        S[rs, pl.ds(own + (w - DIAG), DIAG)] = sd
        m = lane_fold(jnp.maximum, sd)
        if w > DIAG:
            S[rs, pl.ds(own, w - DIAG)] = s[:, :w - DIAG]
            m = jnp.maximum(m, lane_fold(jnp.maximum, s[:, :w - DIAG]))
        mx[rs, :] = m

    diag(score_diag)
    qT[...] = qb[slot].T
    doT[...] = dob[slot].T

    def chunk_a(o):
        for r, n in blocks(RA):
            rs = pl.ds(r, n)
            s = lax.dot_general(qb[slot, rs, :], kb[kv, pl.ds(o, BLK), :], NT, preferred_element_type=F32)
            S[rs, pl.ds(o, BLK)] = s
            mx[rs, :] = jnp.maximum(mx[rs, :], lane_fold(jnp.maximum, s))

    sweep(chunk_a)

    mx[...] = jnp.broadcast_to(jnp.max(mx[...], axis=1, keepdims=True) * SCALE2, (QR, 128))

    def probs(o, w, r, n, first):
        rs = pl.ds(r, n)
        p = jnp.exp2(S[rs, pl.ds(o, w)] * SCALE2 - lanes(mx[rs, :], w))
        S[rs, pl.ds(o, w)] = p
        ls = lane_fold(jnp.add, p)
        oo = jnp.dot(p.astype(BF16), vb[kv, pl.ds(o, w), :], preferred_element_type=F32)
        if first:
            lx[rs, :] = ls
            oacc[rs, :] = oo
        else:
            lx[rs, :] += ls
            oacc[rs, :] += oo

    diag(lambda u, w, r, n: probs(own, w, r, n, True))

    def chunk_b(o):
        for r, n in blocks(RB):
            probs(o, BLK, r, n, False)

    sweep(chunk_b)

    before_pass_c()
    lx[...] = jnp.broadcast_to(1.0 / jnp.sum(lx[...], axis=1, keepdims=True), (QR, 128))
    out = oacc[...] * lx[...]
    ob[oslot] = out.astype(BF16)
    mx[...] = jnp.broadcast_to(jnp.sum(out * dob[slot].astype(F32), axis=1, keepdims=True), (QR, 128))

    def grads(o, w, r, n, late):
        rs = pl.ds(r, n)

        def upstream():
            return lax.dot_general(dob[slot, rs, :], vb[kv, pl.ds(o, w), :], NT, preferred_element_type=F32)

        if late:
            pn = S[rs, pl.ds(o, w)] * lanes(lx[rs, :], w)
            dp = upstream()
        else:
            dp = upstream()
            pn = S[rs, pl.ds(o, w)] * lanes(lx[rs, :], w)
        ds = (pn * (dp - lanes(mx[rs, :], w))).astype(BF16)
        if late:
            gq = jnp.dot(ds, kb[kv, pl.ds(o, w), :], preferred_element_type=F32)
            gk = jnp.dot(qT[:, rs], ds, preferred_element_type=F32)
            gv = jnp.dot(doT[:, rs], pn.astype(BF16), preferred_element_type=F32)
        else:
            gv = jnp.dot(doT[:, rs], pn.astype(BF16), preferred_element_type=F32)
            gk = jnp.dot(qT[:, rs], ds, preferred_element_type=F32)
            gq = jnp.dot(ds, kb[kv, pl.ds(o, w), :], preferred_element_type=F32)
        return gv, gk, gq

    def grads_diag(u, w, r, n):
        gv, gk, gq = grads(own, w, r, n, False)
        oacc[pl.ds(r, n), :] = gq
        acc[aslot, pl.ds(HD, HD), pl.ds(own, w)] += gv
        acc[aslot, pl.ds(0, HD), pl.ds(own, w)] += gk

    diag(grads_diag)
    after_forward()

    @pl.loop(0, blk)
    def _(j):
        o = pl.multiple_of(j * BLK, BLK)
        av, ak = None, None
        for r, n in blocks(RC):
            gv, gk, gq = grads(o, BLK, r, n, True)
            oacc[pl.ds(r, n), :] += gq
            av = gv if av is None else av + gv
            ak = gk if ak is None else ak + gk
        acc[aslot, pl.ds(HD, HD), pl.ds(o, BLK)] += av
        acc[aslot, pl.ds(0, HD), pl.ds(o, BLK)] += ak

    dqb[oslot] = (oacc[...] * SCALE).astype(BF16)


def kernel(q, do, k, v, out, dq, dk, dv, qh, doh, kh, vh, kn, vn, qs, dos, os_, dqs, dks, dvs, l1, la, lb, lc, pp,
           qb, dob, kb, vb, ob, dqb, kst, vst, fin, S, acc, oacc, mx, lx, qT, doT,
           kvsend, kvrecv, swsend, swrecv, hsend, hrecv, rsend, rrecv, load, lout,
           l1r, lar, lbr, lcr, fl, accin, fsend, tin, tout, osend, asend, ssend):
    y = lax.axis_index('ctxo')
    b = lax.axis_index('ctx')
    x = b // 2
    core = lax.rem(b, 2)
    me = y * 4 + b
    chip = 2 * y + x
    other = 2 * chip + 1 - core

    def device(d):
        return (0, d // 4, lax.rem(d, 4))

    def plane(c):
        return 2 * c + core

    def on_chip(c):
        return pl.when(chip == c)

    def partner(step):
        off = lax.rem(2 * step, NDEV) + step // 4
        return (lax.rem(y + off // 4, 2) * 4 + lax.rem(x + lax.rem(off // 2, 2), 2) * 2
                + lax.rem(core + lax.rem(off, 2), 2))

    def remote(source, target, ssem, rsem, dev):
        return pltpu.make_async_remote_copy(src_ref=source, dst_ref=target, send_sem=ssem, recv_sem=rsem,
                                            device_id=device(dev), device_id_type=MESH)

    barrier = pltpu.get_barrier_semaphore()
    for step in range(1, NDEV):
        pl.semaphore_signal(barrier, inc=1, device_id=device(partner(step)), device_id_type=MESH)
    pl.semaphore_wait(barrier, NDEV - 1)

    src = (k, v, q, do)
    hdst = (kh, vh, qh, doh)
    ndst = (kn, vn)
    sdst = (qs, dos)
    bufs = (kb, vb, qb, dob)

    def kv_send(p, blk, kind, dev, own):
        for t in range(2):
            rows = pl.ds(2 * p, 2)
            source = src[t].at[rows] if own else ndst[t].at[rows, blk]
            yield remote(source, ndst[t].at[rows, blk], kvsend.at[t, p, blk // 2, kind], kvrecv.at[t, p, blk], dev)

    def kv_arrived(p, blk):
        for t in range(2):
            view = ndst[t].at[pl.ds(2 * p, 2), blk]
            remote(view, view, kvsend.at[t, p, 0, 0], kvrecv.at[t, p, blk], other).wait_recv()

    def own_kv(p, what):
        for c, targets in ((0, ((1, 0), (2, 2))), (1, ((3, 0),)), (2, ((3, 0),))):
            @on_chip(c)
            def _():
                for cc, kind in targets:
                    for cp in kv_send(p, me, kind, plane(cc), True):
                        what(cp)
        @pl.when((chip == 1) & (p < DIRECT))
        def _():
            for cp in kv_send(p, me, 2, plane(2), True):
                what(cp)

        for cp in kv_send(p, me, 1, other, True):
            what(cp)

    PASS = {1: ((0, 3),), 2: ((0, None), (1, None)), 3: ((1, 2), (2, None), (0, None))}

    def forward(p, c):
        for cs, relay in PASS[c]:
            blk = plane(cs)
            kv_arrived(p, blk)
            if relay is not None:
                @pl.when((p >= DIRECT) | (c == 1))
                def _():
                    for cp in kv_send(p, blk, 0, plane(relay), False):
                        cp.start()

            for cp in kv_send(p, blk, 1, other, False):
                cp.start()

    def forward_done(p, c):
        for cs, relay in PASS[c]:
            blk = plane(cs)
            if relay is not None:
                @pl.when((p >= DIRECT) | (c == 1))
                def _():
                    for cp in kv_send(p, blk, 0, plane(relay), False):
                        cp.wait_send()

            for cp in kv_send(p, blk, 1, other, False):
                cp.wait_send()

    def swap_send(g):
        for t in range(2):
            yield remote(src[2 + t].at[pl.ds(4 * g + 2, 2)], sdst[t].at[pl.ds(2 * g, 2)],
                         swsend.at[t, g], swrecv.at[t, g], other)

    def home_send(hi):
        for t in range(4):
            yield remote(src[t].at[NA + hi], hdst[t].at[HSLOT[hi], me], hsend.at[t, hi], hrecv.at[t, HSLOT[hi], me],
                         HOMES[hi])

    def home_out(hi, what):
        @pl.when(me != HOMES[hi])
        def _():
            for cp in home_send(hi):
                what(cp)

    start = lambda cp: cp.start()
    own_kv(0, start)

    @pl.when(lax.rem(chip, 2) == 0)
    def _():
        @pl.loop(1, NP)
        def _(p):
            own_kv(p, start)

    home_out(EARLY[0], start)
    for c in (1, 2, 3):
        @on_chip(c)
        def _():
            forward(0, c)

    @pl.when(lax.rem(chip, 2) == 1)
    def _():
        own_kv(1, start)

    for g in range(NP // 2):
        for cp in swap_send(g):
            cp.start()
    for hi in EARLY[1:]:
        home_out(hi, start)

    rbuf = (ob, dqb, kst, vst)
    rdst = (out, dq, dk, dv)

    def reply(t, row, i, idx):
        source = rbuf[t].at[idx]
        far = remote(source, rdst[t].at[row], rsend.at[t, idx], rrecv.at[t, row], i)
        near = pltpu.make_async_copy(source, rdst[t].at[row], lout.at[t, idx])
        return far, near

    def reply_start(t, row, i, idx):
        far, near = reply(t, row, i, idx)

        @pl.when(i == me)
        def _():
            near.start()

        @pl.when(i != me)
        def _():
            far.start()

    def reply_wait(t, row, i, idx):
        far, near = reply(t, row, i, idx)

        @pl.when(i == me)
        def _():
            near.wait()

        @pl.when(i != me)
        def _():
            far.wait_send()

    def tmp(idx):
        return S.at[pl.ds(2 * HD * idx, 2 * HD), pl.ds(0, BLK)]

    def take(source, idx):
        return pltpu.make_async_copy(source, tmp(idx), tin.at[idx])

    def piece(aslot, j):
        return acc.at[aslot, :, pl.ds(pl.multiple_of(j * BLK, BLK), BLK)]

    def pair_out(p, j):
        return remote(piece(0, j), l1.at[p, j], fl.at[0, j], l1r.at[p, j], other)

    def row_keep(p, j):
        return pltpu.make_async_copy(piece(1, j), pp.at[p, j], fl.at[1, j])

    def kept(c):
        return range(6 if c == 3 else 2 * c + 2)

    def row_send(p, c, j):
        target = {3: {0: (la, 0, lar, 1), 1: (la, 1, lar, 1), 2: (la, 2, lar, 1), 3: (la, 3, lar, 1),
                      4: (la, 0, lar, 2), 5: (la, 1, lar, 2)},
                  2: {0: (lb, 0, lbr, 0), 1: (lb, 1, lbr, 0), 2: (la, 0, lar, 3), 3: (la, 1, lar, 3)}}[c]
        land, idx, sem, cc = target[j]
        return remote(pp.at[p, j], land.at[p, idx], osend.at[p, j], sem.at[p, idx], plane(cc))

    SENT = {3: (4, 5, 0, 1), 2: (2, 3, 0, 1)}

    def rows_leave(p):
        for c in range(4):
            @on_chip(c)
            def _():
                for j in kept(c):
                    row_keep(p, j).wait()
                for j in SENT.get(c, ()):
                    if c == 3 and j < 2:
                        @pl.when(p < NP - 1)
                        def _():
                            row_send(p, c, j).start()

                        @pl.when(p == NP - 1)
                        def _():
                            last_direct(j).start()
                    else:
                        row_send(p, c, j).start()
                if c == 1:
                    @pl.when(p == NP - 1)
                    def _():
                        for j in range(2):
                            last_onward(j).start()

    def last_direct(j):
        return remote(pp.at[NP - 1, j], lc.at[j], osend.at[NP - 1, j], lcr.at[j], plane(0))

    def last_onward(j):
        return remote(pp.at[NP - 1, j], la.at[NP - 1, j], osend.at[NP - 1, j], lar.at[NP - 1, j], plane(0))

    def rows_left(p):
        for c, js in ((3, range(6)), (2, range(4))):
            @on_chip(c)
            def _():
                for j in js:
                    row_send(p, c, j).wait_send()

        @pl.when((chip == 1) & (p == NP - 1))
        def _():
            for j in range(2):
                last_onward(j).wait_send()

    def join_chip2(p):
        for j in (2, 3):
            la_arrived(p, j - 2)
            take(pp.at[p, j], 2 * j - 4).start()
            take(la.at[p, j - 2], 2 * j - 3).start()
        for j in (2, 3):
            a, b = 2 * j - 4, 2 * j - 3
            take(pp.at[p, j], a).wait()
            take(la.at[p, j - 2], b).wait()
            tmp(a)[...] += tmp(b)[...]
            pltpu.make_async_copy(tmp(a), pp.at[p, j], tout.at[j - 2]).start()
        for j in (2, 3):
            pltpu.make_async_copy(tmp(2 * j - 4), pp.at[p, j], tout.at[j - 2]).wait()
            row_send(p, 3, j).start()

    def la_arrived(p, j):
        remote(la.at[p, j], la.at[p, j], fl.at[0, 0], lar.at[p, j], other).wait_recv()

    def lb_arrived(p, j):
        remote(lb.at[p, j], lb.at[p, j], fl.at[0, 0], lbr.at[p, j], other).wait_recv()

    def fin_copies(p, kk):
        row = 2 * p + core
        for t in range(2):
            yield (remote(fin.at[kk, t], rdst[2 + t].at[row], fsend.at[kk, t], rrecv.at[2 + t, row], other),
                   pltpu.make_async_copy(fin.at[kk, t], rdst[2 + t].at[row], fsend.at[kk, t]))

    def fin_wait(p, kk):
        for far, near in fin_copies(p, kk):
            @pl.when(core == kk)
            def _():
                near.wait()

            @pl.when(core != kk)
            def _():
                far.wait_send()

    def finish(p, kk, g):
        @pl.when(p > 0)
        def _():
            fin_wait(p - 1, kk)

        fin[kk, 0] = (g[:HD] * SCALE).T.astype(BF16)
        fin[kk, 1] = g[HD:].T.astype(BF16)
        for far, near in fin_copies(p, kk):
            @pl.when(core == kk)
            def _():
                near.start()

            @pl.when(core != kk)
            def _():
                far.start()

    def task_row(task):
        p = task // 2
        row = 2 * p + lax.rem(1 - core + lax.rem(task, 2), 2)
        i = 2 * chip + lax.rem(core + lax.rem(p, 2), 2)
        return row, i

    def kv_slot(t, slot, blk):
        return bufs[t].at[slot, pl.ds(pl.multiple_of(blk * BLK, BLK), BLK), :]

    def fetch(task):
        p = task // 2
        slot = lax.rem(task, 2)
        row, i = task_row(task)

        @pl.when(slot == 0)
        def _():
            @pl.loop(0, chip + 1)
            def _(cs):
                kv_arrived(p, 2 * cs + 1 - core)

            @pl.when(i != me)
            def _():
                for cp in swap_send(p // 2):
                    cp.wait_recv()

        @pl.loop(0, 2 * chip + 2)
        def _(blk):
            @pl.when(blk == me)
            def _():
                for t in range(2):
                    pltpu.make_async_copy(src[t].at[row], kv_slot(t, slot, blk), load.at[t, blk]).start()

            @pl.when(blk != me)
            def _():
                for t in range(2):
                    pltpu.make_async_copy(ndst[t].at[row, blk], kv_slot(t, slot, blk), load.at[t, blk]).start()

        @pl.when(i == me)
        def _():
            for t in (2, 3):
                pltpu.make_async_copy(src[t].at[row], bufs[t].at[slot], load.at[t, 0]).start()

        @pl.when(i != me)
        def _():
            for t in (2, 3):
                pltpu.make_async_copy(sdst[t - 2].at[2 * (p // 2) + lax.rem(row, 2)], bufs[t].at[slot],
                                      load.at[t, 0]).start()

    def fetch_wait(task):
        slot = lax.rem(task, 2)

        @pl.loop(0, 2 * chip + 2)
        def _(blk):
            for t in range(2):
                pltpu.make_async_copy(ndst[t].at[0, blk], kv_slot(t, slot, blk), load.at[t, blk]).wait()

        for t in (2, 3):
            pltpu.make_async_copy(src[t].at[0], bufs[t].at[slot], load.at[t, 0]).wait()

    fetch(0)

    @pl.loop(0, NA)
    def _(task):
        p = task // 2
        slot = lax.rem(task, 2)
        oslot = lax.rem(task, NSLOT)
        row, i = task_row(task)

        @pl.when((task + 2 < NP) & (lax.rem(chip, 2) == 1))
        def _():
            own_kv(task + 2, start)

        for when, rows in enumerate(LATER):
            @pl.when(task == when)
            def _():
                for hi in rows:
                    home_out(hi, start)

        fetch_wait(task)

        @pl.when((slot == 0) & (p > 0))
        def _():
            rows_leave(p - 1)

        @pl.when(task >= NSLOT)
        def _():
            row0, i0 = task_row(task - NSLOT)
            reply_wait(0, row0, i0, oslot)
            reply_wait(1, row0, i0, oslot)

        def after_forward():
            reply_start(0, row, i, oslot)

        def before_pass_c():
            @pl.when((chip == 1) & (task + 1 < NP))
            def _():
                forward(task + 1, 1)

            @pl.when((chip == 2) & (slot == 1) & (p + 1 < NP))
            def _():
                forward(p + 1, 2)

            @pl.when((chip == 3) & (task > 0) & (task < NP))
            def _():
                forward(task, 3)

            @pl.when(task + 1 < NA)
            def _():
                fetch(task + 1)

            @pl.when(slot == 0)
            def _():
                @pl.when(p > 0)
                def _():
                    @pl.loop(0, 2 * chip + 2)
                    def _(j):
                        pair_out(p - 1, j).wait_send()

                acc[0] = jnp.zeros((2 * HD, SEQ), F32)

            @pl.when(slot == 1)
            def _():
                @pl.loop(0, 2 * chip + 2)
                def _(j):
                    pair_out(p, j).wait_recv()
                    pltpu.make_async_copy(l1.at[p, j], piece(1, j), accin.at[j]).start()

                @pl.loop(0, 2 * chip + 2)
                def _(j):
                    pltpu.make_async_copy(l1.at[p, j], piece(1, j), accin.at[j]).wait()

        attn_tile(i, slot, oslot, slot, qb, dob, kb, vb, ob, dqb, S, acc, slot, oacc, mx, lx, qT, doT,
                  after_forward, before_pass_c)
        reply_start(1, row, i, oslot)

        @pl.when(slot == 0)
        def _():
            @pl.loop(0, 2 * chip + 2)
            def _(j):
                pair_out(p, j).start()

        @pl.when((slot == 0) & (p > 0) & (chip == 3))
        def _():
            join_chip2(p - 1)

        @pl.when(slot == 1)
        def _():
            for c in range(4):
                @on_chip(c)
                def _():
                    for j in kept(c):
                        row_keep(p, j).start()
                    if c == 3:
                        for kk in range(2):
                            finish(p, kk, acc[1, :, pl.ds((6 + kk) * BLK, BLK)])

    @pl.loop(NA - NSLOT, NA)
    def _(task):
        row0, i0 = task_row(task)
        reply_wait(0, row0, i0, lax.rem(task, NSLOT))
        reply_wait(1, row0, i0, lax.rem(task, NSLOT))

    @pl.loop(0, 2 * chip + 2)
    def _(j):
        pair_out(NP - 1, j).wait_send()

    rows_leave(NP - 1)

    @on_chip(3)
    def _():
        join_chip2(NP - 1)

    def pick(values):
        got = jnp.int32(values[0])
        for d in range(1, NDEV):
            got = jnp.where(me == d, values[d], got)
        return got

    hcount = pick([HOMES.count(d) for d in range(NDEV)])
    first = pick([HOMES.index(d) if d in HOMES else 0 for d in range(NDEV)])

    def home_block(step):
        return lax.rem(2 * chip - 1 - step + NDEV, NDEV)

    def home_row(h):
        return NA + first + h

    def home_arrived(t, h, i):
        view = hdst[t].at[h, i]
        remote(view, view, hsend.at[t, 0], hrecv.at[t, h, i], other).wait_recv()

    def home_kv(h):
        row = home_row(h)
        for t in range(2):
            pltpu.make_async_copy(src[t].at[row], kv_slot(t, h, me), load.at[t, me]).start()

        @pl.loop(1, NDEV)
        def _(step):
            i = partner(step)
            for t in range(2):
                home_arrived(t, h, i)
                pltpu.make_async_copy(hdst[t].at[h, i], kv_slot(t, h, i), load.at[t, i]).start()

        @pl.loop(0, NDEV)
        def _(i):
            for t in range(2):
                pltpu.make_async_copy(hdst[t].at[h, i], kv_slot(t, h, i), load.at[t, i]).wait()

    def home_fetch(task):
        h = task // NDEV
        step = lax.rem(task, NDEV)
        slot = lax.rem(task, 2)
        i = home_block(step)

        @pl.when(i == me)
        def _():
            for t in (2, 3):
                pltpu.make_async_copy(src[t].at[home_row(h)], bufs[t].at[slot], load.at[t, 0]).start()

        @pl.when(i != me)
        def _():
            for t in (2, 3):
                home_arrived(t, h, i)
                pltpu.make_async_copy(hdst[t].at[h, i], bufs[t].at[slot], load.at[t, 0]).start()

    def home_task(task):
        return home_row(task // NDEV), home_block(lax.rem(task, NDEV))

    stage = (os_, dqs)
    sstage = (dks, dvs)

    def put_down(t, task):
        row, i = home_task(task)
        idx = lax.rem(task, NSLOT)
        return (pltpu.make_async_copy(rbuf[t].at[idx], rdst[t].at[row], lout.at[t, idx]),
                pltpu.make_async_copy(rbuf[t].at[idx], stage[t].at[task], lout.at[t, idx]))

    def put_down_start(t, task):
        own, put = put_down(t, task)
        i = home_task(task)[1]

        @pl.when(i == me)
        def _():
            own.start()

        @pl.when(i != me)
        def _():
            put.start()

    def away(t, task):
        row, i = home_task(task)
        return remote(stage[t].at[task], rdst[t].at[row], asend.at[t, task], rrecv.at[t, row], i)

    def send_away(t, task):
        own, put = put_down(t, task)
        i = home_task(task)[1]

        @pl.when(i == me)
        def _():
            own.wait()

        @pl.when(i != me)
        def _():
            put.wait()
            away(t, task).start()

    def sum_down(t, h, j, away_too):
        target = sstage[t - 2].at[h, j] if away_too else rdst[t].at[home_row(h)]
        return pltpu.make_async_copy(rbuf[t], target, lout.at[t, 0])

    def sum_away(t, h, j):
        row = home_row(h)
        return remote(sstage[t - 2].at[h, j], rdst[t].at[row], ssend.at[t - 2, h, j], rrecv.at[t, row], j)

    @pl.when(hcount > 0)
    def _():
        home_fetch(0)

    @pl.loop(0, NDEV * hcount)
    def _(task):
        h = task // NDEV
        step = lax.rem(task, NDEV)
        slot = lax.rem(task, 2)
        oslot = lax.rem(task, NSLOT)
        row, i = home_task(task)

        @pl.when(step == 0)
        def _():
            home_kv(h)
            acc[h] = jnp.zeros((2 * HD, SEQ), F32)

        for t in (2, 3):
            pltpu.make_async_copy(src[t].at[0], bufs[t].at[slot], load.at[t, 0]).wait()

        @pl.when(task > 0)
        def _():
            send_away(1, task - 1)

        def after_forward():
            put_down_start(0, task)

        def before_pass_c():
            @pl.when(task + 1 < NDEV * hcount)
            def _():
                home_fetch(task + 1)

        attn_tile(i, slot, oslot, h, qb, dob, kb, vb, ob, dqb, S, acc, h, oacc, mx, lx, qT, doT,
                  after_forward, before_pass_c)
        put_down_start(1, task)
        send_away(0, task)

        def flush(j):
            o = pl.ds(pl.multiple_of(j * BLK, BLK), BLK)
            kst[...] = (acc[h, pl.ds(0, HD), o] * SCALE).T.astype(BF16)
            vst[...] = acc[h, pl.ds(HD, HD), o].T.astype(BF16)
            for where, away_too in ((j == me, False), (j != me, True)):
                @pl.when(where)
                def _():
                    for t in (2, 3):
                        sum_down(t, h, j, away_too).start()
                    for t in (2, 3):
                        sum_down(t, h, j, away_too).wait()
                        if away_too:
                            sum_away(t, h, j).start()

        @pl.when(step >= 2 * chip)
        def _():
            flush(i)

        @pl.when(step == NDEV - 1)
        def _():
            @pl.loop(0, 2 * chip)
            def _(j):
                flush(j)

    @pl.when(hcount > 0)
    def _():
        send_away(1, NDEV * hcount - 1)

    @pl.loop(0, NP)
    def _(p):
        @on_chip(1)
        def _():
            def join(j):
                la_arrived(p, j)
                take(pp.at[p, j], 0).start()
                take(la.at[p, j], 1).start()
                take(pp.at[p, j], 0).wait()
                take(la.at[p, j], 1).wait()

            for j in range(2):
                onward = lambda pq: remote(tmp(2 + j), la.at[pq, j], tout.at[j], lar.at[pq, j], plane(0))

                @pl.when(p > 0)
                def _():
                    onward(p - 1).wait_send()

                @pl.when(p < NP - 1)
                def _():
                    join(j)
                    tmp(2 + j)[...] = tmp(0)[...] + tmp(1)[...]
                    onward(p).start()

            for j in (2, 3):
                join(j)
                finish(p, j - 2, tmp(0)[...] + tmp(1)[...])

        @on_chip(2)
        def _():
            for j in range(2):
                la_arrived(p, j)
                take(pp.at[p, 4 + j], 2 * j).start()
                take(la.at[p, j], 2 * j + 1).start()
                take(pp.at[p, 4 + j], 2 * j).wait()
                take(la.at[p, j], 2 * j + 1).wait()
                finish(p, j, tmp(2 * j)[...] + tmp(2 * j + 1)[...])

        @on_chip(0)
        def _():
            for j in range(2):
                la_arrived(p, j)
                lb_arrived(p, j)
                take(pp.at[p, j], 0).start()
                take(la.at[p, j], 1).start()
                take(lb.at[p, j], 2).start()
                take(pp.at[p, j], 0).wait()
                take(la.at[p, j], 1).wait()
                take(lb.at[p, j], 2).wait()

                @pl.when(p == NP - 1)
                def _():
                    remote(lc.at[j], lc.at[j], fl.at[0, 0], lcr.at[j], other).wait_recv()
                    take(lc.at[j], 3).start()
                    take(lc.at[j], 3).wait()
                    tmp(2)[...] += tmp(3)[...]

                finish(p, j, tmp(0)[...] + tmp(1)[...] + tmp(2)[...])

    for kk in range(2):
        fin_wait(NP - 1, kk)

    finished = lambda cp: cp.wait_send()

    @pl.loop(0, NP)
    def _(p):
        own_kv(p, finished)
        rows_left(p)
        for c in (1, 2, 3):
            @on_chip(c)
            def _():
                forward_done(p, c)

    @pl.loop(0, NDEV * hcount)
    def _(task):
        @pl.when(home_task(task)[1] != me)
        def _():
            away(0, task).wait_send()
            away(1, task).wait_send()
            for t in (2, 3):
                sum_away(t, task // NDEV, home_task(task)[1]).wait_send()

    for g in range(NP // 2):
        for cp in swap_send(g):
            cp.wait_send()
    for hi in range(len(HOMES)):
        home_out(hi, finished)

    def came(t, row):
        source = rbuf[t].at[0] if t < 2 else rbuf[t]
        remote(source, rdst[t].at[row], rsend.at[t, 0], rrecv.at[t, row], other).wait_recv()

    for hi in range(len(HOMES)):
        @pl.when(me != HOMES[hi])
        def _():
            for t in range(4):
                came(t, NA + hi)

    @pl.loop(0, NA)
    def _(row):
        @pl.when(lax.rem(row // 2, 2) == 1)
        def _():
            came(0, row)
            came(1, row)

        @pl.when(lax.rem(row, 2) != core)
        def _():
            came(2, row)
            came(3, row)


def solution(mesh):
    spec = P('data', ('ctxo', 'ctx'), None, None)
    any_spec = pl.BlockSpec(memory_space=pl.ANY)

    def local_attn(q_in, k_in, v_in, do_in):
        rows = q_in.shape[0]
        wide = (QR, HD)
        narrow = (BLK, HD)
        shape = lambda lead, tail, dtype=BF16: jax.ShapeDtypeStruct(lead + tail, dtype)
        pair = (2 * HD, BLK)
        vmem = pltpu.VMEM
        dma = pltpu.SemaphoreType.DMA
        call = pl.pallas_call(
            kernel,
            out_shape=[
                shape((rows,), wide), shape((rows,), wide), shape((rows,), narrow), shape((rows,), narrow),
                shape((2, NDEV), wide), shape((2, NDEV), wide), shape((2, NDEV), narrow), shape((2, NDEV), narrow),
                shape((NA, NDEV), narrow), shape((NA, NDEV), narrow), shape((NP,), wide), shape((NP,), wide),
                shape((2 * NDEV,), wide), shape((2 * NDEV,), wide),
                shape((2, NDEV), narrow), shape((2, NDEV), narrow),
                shape((NP, NDEV), pair, F32), shape((NP, 4), pair, F32), shape((NP, 2), pair, F32), shape((2,), pair, F32),
                shape((NP, 6), pair, F32),
            ],
            in_specs=[any_spec] * 4,
            out_specs=[any_spec] * 21,
            scratch_shapes=[
                vmem((2,) + wide, BF16), vmem((2,) + wide, BF16),
                vmem((2, SEQ, HD), BF16), vmem((2, SEQ, HD), BF16),
                vmem((NSLOT,) + wide, BF16), vmem((NSLOT,) + wide, BF16),
                vmem((BLK, HD), BF16), vmem((BLK, HD), BF16),
                vmem((2, 2) + narrow, BF16),
                vmem((QR, SEQ), F32), vmem((2, 2 * HD, SEQ), F32),
                vmem((QR, HD), F32),
                vmem((QR, 128), F32), vmem((QR, 128), F32),
                vmem((HD, QR), BF16), vmem((HD, QR), BF16),
                dma((2, NP, 4, 3)), dma((2, NP, NDEV)), dma((2, NP // 2)), dma((2, NP // 2)),
                dma((4, len(HOMES))), dma((4, 2, NDEV)), dma((2, NSLOT)), dma((4, rows)), dma((4, NDEV)), dma((4, NSLOT)),
                dma((NP, NDEV)), dma((NP, 4)), dma((NP, 2)), dma((2,)), dma((2, NDEV)), dma((NDEV,)), dma((2, 2)),
                dma((4,)), dma((2,)), dma((NP, 6)), dma((2, 2 * NDEV)), dma((2, 2, NDEV)),
            ],
            compiler_params=pltpu.CompilerParams(
                collective_id=0, has_side_effects=True, vmem_limit_bytes=67043328),
        )
        res = call(q_in.reshape((rows,) + wide), do_in.reshape((rows,) + wide),
                   k_in.reshape((rows,) + narrow), v_in.reshape((rows,) + narrow))
        return (res[0].reshape(q_in.shape), res[1].reshape(q_in.shape),
                res[2].reshape(k_in.shape), res[3].reshape(v_in.shape))

    return jax.shard_map(local_attn, mesh=mesh, in_specs=(spec,) * 4, out_specs=(spec,) * 4, check_vma=False)
```

```python
import functools
import math

import jax
import jax.numpy as jnp
from jax import lax
from jax.experimental import pallas as pl
from jax.experimental.pallas import tpu as pltpu
from jax.sharding import PartitionSpec as P

MESH = pl.DeviceIdType.MESH
NT = (((1,), (1,)), ((), ()))
F32 = jnp.float32
BF16 = jnp.bfloat16
NDEV = 8
BLK = 512
QR = 4 * BLK
HD = 128
SEQ = NDEV * BLK
SCALE = 1.0 / math.sqrt(HD)
SCALE2 = SCALE * math.log2(math.e)
DIAG = 256
RA = 1024
RB = 1024
RC = 1024
NSLOT = 2
NA = 10
NP = NA // 2
LAST = 2
DIRECT = 5
HOMES = (0, 0, 1, 2, 4, 5)
HSLOT = (0, 1, 0, 0, 0, 0)
EARLY = (0, 3, 2)
LATER = ((), (), (), (1,), (4, 5))


def lane_fold(op, s):
    acc = s[:, 0:128]
    for g in range(1, s.shape[1] // 128):
        acc = op(acc, s[:, g * 128:(g + 1) * 128])
    return acc


def lanes(x, width):
    return jnp.tile(x, (1, width // 128))


def attn_tile(blk, slot, oslot, kv, qb, dob, kb, vb, ob, dqb, S, acc, aslot, oacc, mx, lx, qT, doT, after_forward, before_pass_c):
    own = pl.multiple_of(blk * BLK, BLK)
    blocks = lambda n: [(r, n) for r in range(0, QR, n)]

    def diag(fn):
        for u in reversed(range(BLK // DIAG)):
            fn(u, DIAG * (u + 1), u * DIAG * 4, DIAG * 4)

    def sweep(chunk):
        @pl.loop(0, blk // 2)
        def _(j):
            chunk(pl.multiple_of(2 * j * BLK, BLK))
            chunk(pl.multiple_of((2 * j + 1) * BLK, BLK))

        @pl.when(lax.rem(blk, 2) == 1)
        def _():
            chunk(pl.multiple_of((blk - 1) * BLK, BLK))

    def score_diag(u, w, r, n):
        rs = pl.ds(r, n)
        s = lax.dot_general(qb[slot, rs, :], kb[kv, pl.ds(own, w), :], NT, preferred_element_type=F32)
        row = lax.broadcasted_iota(jnp.int32, (n, DIAG), 0) // 4
        col = lax.broadcasted_iota(jnp.int32, (n, DIAG), 1)
        sd = jnp.where(row >= col, s[:, w - DIAG:], -1e30)
        S[rs, pl.ds(own + (w - DIAG), DIAG)] = sd
        m = lane_fold(jnp.maximum, sd)
        if w > DIAG:
            S[rs, pl.ds(own, w - DIAG)] = s[:, :w - DIAG]
            m = jnp.maximum(m, lane_fold(jnp.maximum, s[:, :w - DIAG]))
        mx[rs, :] = m

    diag(score_diag)
    qT[...] = qb[slot].T
    doT[...] = dob[slot].T

    def chunk_a(o):
        for r, n in blocks(RA):
            rs = pl.ds(r, n)
            s = lax.dot_general(qb[slot, rs, :], kb[kv, pl.ds(o, BLK), :], NT, preferred_element_type=F32)
            S[rs, pl.ds(o, BLK)] = s
            mx[rs, :] = jnp.maximum(mx[rs, :], lane_fold(jnp.maximum, s))

    sweep(chunk_a)

    mx[...] = jnp.broadcast_to(jnp.max(mx[...], axis=1, keepdims=True) * SCALE2, (QR, 128))

    def probs(o, w, r, n, first):
        rs = pl.ds(r, n)
        p = jnp.exp2(S[rs, pl.ds(o, w)] * SCALE2 - lanes(mx[rs, :], w))
        S[rs, pl.ds(o, w)] = p
        ls = lane_fold(jnp.add, p)
        oo = jnp.dot(p.astype(BF16), vb[kv, pl.ds(o, w), :], preferred_element_type=F32)
        if first:
            lx[rs, :] = ls
            oacc[rs, :] = oo
        else:
            lx[rs, :] += ls
            oacc[rs, :] += oo

    diag(lambda u, w, r, n: probs(own, w, r, n, True))

    def chunk_b(o):
        for r, n in blocks(RB):
            probs(o, BLK, r, n, False)

    sweep(chunk_b)

    before_pass_c()
    lx[...] = jnp.broadcast_to(1.0 / jnp.sum(lx[...], axis=1, keepdims=True), (QR, 128))
    out = oacc[...] * lx[...]
    ob[oslot] = out.astype(BF16)
    mx[...] = jnp.broadcast_to(jnp.sum(out * dob[slot].astype(F32), axis=1, keepdims=True), (QR, 128))

    def grads(o, w, r, n, late):
        rs = pl.ds(r, n)

        def upstream():
            return lax.dot_general(dob[slot, rs, :], vb[kv, pl.ds(o, w), :], NT, preferred_element_type=F32)

        if late:
            pn = S[rs, pl.ds(o, w)] * lanes(lx[rs, :], w)
            dp = upstream()
        else:
            dp = upstream()
            pn = S[rs, pl.ds(o, w)] * lanes(lx[rs, :], w)
        ds = (pn * (dp - lanes(mx[rs, :], w))).astype(BF16)
        if late:
            gq = jnp.dot(ds, kb[kv, pl.ds(o, w), :], preferred_element_type=F32)
            gk = jnp.dot(qT[:, rs], ds, preferred_element_type=F32)
            gv = jnp.dot(doT[:, rs], pn.astype(BF16), preferred_element_type=F32)
        else:
            gv = jnp.dot(doT[:, rs], pn.astype(BF16), preferred_element_type=F32)
            gk = jnp.dot(qT[:, rs], ds, preferred_element_type=F32)
            gq = jnp.dot(ds, kb[kv, pl.ds(o, w), :], preferred_element_type=F32)
        return gv, gk, gq

    def grads_diag(u, w, r, n):
        gv, gk, gq = grads(own, w, r, n, False)
        oacc[pl.ds(r, n), :] = gq
        acc[aslot, pl.ds(HD, HD), pl.ds(own, w)] += gv
        acc[aslot, pl.ds(0, HD), pl.ds(own, w)] += gk

    diag(grads_diag)
    after_forward()

    @pl.loop(0, blk)
    def _(j):
        o = pl.multiple_of(j * BLK, BLK)
        av, ak = None, None
        for r, n in blocks(RC):
            gv, gk, gq = grads(o, BLK, r, n, True)
            oacc[pl.ds(r, n), :] += gq
            av = gv if av is None else av + gv
            ak = gk if ak is None else ak + gk
        acc[aslot, pl.ds(HD, HD), pl.ds(o, BLK)] += av
        acc[aslot, pl.ds(0, HD), pl.ds(o, BLK)] += ak

    dqb[oslot] = (oacc[...] * SCALE).astype(BF16)


def kernel(q, do, k, v, out, dq, dk, dv, qh, doh, kh, vh, kn, vn, qs, dos, os_, dqs, dks, dvs, l1, la, lb, lc, pp,
           qb, dob, kb, vb, ob, dqb, kst, vst, fin, S, acc, oacc, mx, lx, qT, doT,
           kvsend, kvrecv, swsend, swrecv, hsend, hrecv, rsend, rrecv, load, lout,
           l1r, lar, lbr, lcr, fl, accin, fsend, tin, tout, osend, asend, ssend):
    y = lax.axis_index('ctxo')
    b = lax.axis_index('ctx')
    x = b // 2
    core = lax.rem(b, 2)
    me = y * 4 + b
    chip = 2 * y + x
    other = 2 * chip + 1 - core

    def device(d):
        return (0, d // 4, lax.rem(d, 4))

    def plane(c):
        return 2 * c + core

    def on_chip(c):
        return pl.when(chip == c)

    def partner(step):
        off = lax.rem(2 * step, NDEV) + step // 4
        return (lax.rem(y + off // 4, 2) * 4 + lax.rem(x + lax.rem(off // 2, 2), 2) * 2
                + lax.rem(core + lax.rem(off, 2), 2))

    def remote(source, target, ssem, rsem, dev):
        return pltpu.make_async_remote_copy(src_ref=source, dst_ref=target, send_sem=ssem, recv_sem=rsem,
                                            device_id=device(dev), device_id_type=MESH)

    barrier = pltpu.get_barrier_semaphore()
    for step in range(1, NDEV):
        pl.semaphore_signal(barrier, inc=1, device_id=device(partner(step)), device_id_type=MESH)
    pl.semaphore_wait(barrier, NDEV - 1)

    src = (k, v, q, do)
    hdst = (kh, vh, qh, doh)
    ndst = (kn, vn)
    sdst = (qs, dos)
    bufs = (kb, vb, qb, dob)

    def kv_send(p, blk, kind, dev, own):
        for t in range(2):
            rows = pl.ds(2 * p, 2)
            source = src[t].at[rows] if own else ndst[t].at[rows, blk]
            yield remote(source, ndst[t].at[rows, blk], kvsend.at[t, p, blk // 2, kind], kvrecv.at[t, p, blk], dev)

    def kv_arrived(p, blk):
        for t in range(2):
            view = ndst[t].at[pl.ds(2 * p, 2), blk]
            remote(view, view, kvsend.at[t, p, 0, 0], kvrecv.at[t, p, blk], other).wait_recv()

    def own_kv(p, what):
        for c, targets in ((0, ((1, 0), (2, 2))), (1, ((3, 0),)), (2, ((3, 0),))):
            @on_chip(c)
            def _():
                for cc, kind in targets:
                    for cp in kv_send(p, me, kind, plane(cc), True):
                        what(cp)
        @pl.when((chip == 1) & (p < DIRECT))
        def _():
            for cp in kv_send(p, me, 2, plane(2), True):
                what(cp)

        for cp in kv_send(p, me, 1, other, True):
            what(cp)

    PASS = {1: ((0, 3),), 2: ((0, None), (1, None)), 3: ((1, 2), (2, None), (0, None))}

    def forward(p, c):
        for cs, relay in PASS[c]:
            blk = plane(cs)
            kv_arrived(p, blk)
            if relay is not None:
                @pl.when((p >= DIRECT) | (c == 1))
                def _():
                    for cp in kv_send(p, blk, 0, plane(relay), False):
                        cp.start()

            for cp in kv_send(p, blk, 1, other, False):
                cp.start()

    def forward_done(p, c):
        for cs, relay in PASS[c]:
            blk = plane(cs)
            if relay is not None:
                @pl.when((p >= DIRECT) | (c == 1))
                def _():
                    for cp in kv_send(p, blk, 0, plane(relay), False):
                        cp.wait_send()

            for cp in kv_send(p, blk, 1, other, False):
                cp.wait_send()

    def swap_send(g):
        for t in range(2):
            yield remote(src[2 + t].at[pl.ds(4 * g + 2, 2)], sdst[t].at[pl.ds(2 * g, 2)],
                         swsend.at[t, g], swrecv.at[t, g], other)

    def home_send(hi):
        for t in range(4):
            yield remote(src[t].at[NA + hi], hdst[t].at[HSLOT[hi], me], hsend.at[t, hi], hrecv.at[t, HSLOT[hi], me],
                         HOMES[hi])

    def home_out(hi, what):
        @pl.when(me != HOMES[hi])
        def _():
            for cp in home_send(hi):
                what(cp)

    start = lambda cp: cp.start()
    own_kv(0, start)

    @pl.when(lax.rem(chip, 2) == 0)
    def _():
        @pl.loop(1, NP)
        def _(p):
            own_kv(p, start)

    home_out(EARLY[0], start)
    for c in (1, 2, 3):
        @on_chip(c)
        def _():
            forward(0, c)

    @pl.when(lax.rem(chip, 2) == 1)
    def _():
        own_kv(1, start)

    for g in range(NP // 2):
        for cp in swap_send(g):
            cp.start()
    for hi in EARLY[1:]:
        home_out(hi, start)

    rbuf = (ob, dqb, kst, vst)
    rdst = (out, dq, dk, dv)

    def reply(t, row, i, idx):
        source = rbuf[t].at[idx]
        far = remote(source, rdst[t].at[row], rsend.at[t, idx], rrecv.at[t, row], i)
        near = pltpu.make_async_copy(source, rdst[t].at[row], lout.at[t, idx])
        return far, near

    def reply_start(t, row, i, idx):
        far, near = reply(t, row, i, idx)

        @pl.when(i == me)
        def _():
            near.start()

        @pl.when(i != me)
        def _():
            far.start()

    def reply_wait(t, row, i, idx):
        far, near = reply(t, row, i, idx)

        @pl.when(i == me)
        def _():
            near.wait()

        @pl.when(i != me)
        def _():
            far.wait_send()

    def tmp(idx):
        return S.at[pl.ds(2 * HD * idx, 2 * HD), pl.ds(0, BLK)]

    def take(source, idx):
        return pltpu.make_async_copy(source, tmp(idx), tin.at[idx])

    def piece(aslot, j):
        return acc.at[aslot, :, pl.ds(pl.multiple_of(j * BLK, BLK), BLK)]

    def pair_out(p, j):
        return remote(piece(0, j), l1.at[p, j], fl.at[0, j], l1r.at[p, j], other)

    def row_keep(p, j):
        return pltpu.make_async_copy(piece(1, j), pp.at[p, j], fl.at[1, j])

    def kept(c):
        return range(6 if c == 3 else 2 * c + 2)

    def row_send(p, c, j):
        target = {3: {0: (la, 0, lar, 1), 1: (la, 1, lar, 1), 2: (la, 2, lar, 1), 3: (la, 3, lar, 1),
                      4: (la, 0, lar, 2), 5: (la, 1, lar, 2)},
                  2: {0: (lb, 0, lbr, 0), 1: (lb, 1, lbr, 0), 2: (la, 0, lar, 3), 3: (la, 1, lar, 3)}}[c]
        land, idx, sem, cc = target[j]
        return remote(pp.at[p, j], land.at[p, idx], osend.at[p, j], sem.at[p, idx], plane(cc))

    SENT = {3: (4, 5, 0, 1), 2: (2, 3, 0, 1)}

    def rows_leave(p):
        for c in range(4):
            @on_chip(c)
            def _():
                for j in kept(c):
                    row_keep(p, j).wait()
                for j in SENT.get(c, ()):
                    if c == 3 and j < 2:
                        @pl.when(p < NP - LAST)
                        def _():
                            row_send(p, c, j).start()

                        @pl.when(p >= NP - LAST)
                        def _():
                            last_direct(p, j).start()
                    else:
                        row_send(p, c, j).start()
                if c == 1:
                    @pl.when(p >= NP - LAST)
                    def _():
                        for j in range(2):
                            last_onward(p, j).start()

    def last_direct(p, j):
        return remote(pp.at[p, j], lc.at[p - (NP - LAST), j], osend.at[p, j], lcr.at[p - (NP - LAST), j], plane(0))

    def last_onward(p, j):
        return remote(pp.at[p, j], la.at[p, j], osend.at[p, j], lar.at[p, j], plane(0))

    def rows_left(p):
        for c, js in ((3, range(6)), (2, range(4))):
            @on_chip(c)
            def _():
                for j in js:
                    row_send(p, c, j).wait_send()

        @pl.when((chip == 1) & (p >= NP - LAST))
        def _():
            for j in range(2):
                last_onward(p, j).wait_send()

    def join_chip2(p):
        for j in (2, 3):
            la_arrived(p, j - 2)
            take(pp.at[p, j], 2 * j - 4).start()
            take(la.at[p, j - 2], 2 * j - 3).start()
        for j in (2, 3):
            a, b = 2 * j - 4, 2 * j - 3
            take(pp.at[p, j], a).wait()
            take(la.at[p, j - 2], b).wait()
            tmp(a)[...] += tmp(b)[...]
            pltpu.make_async_copy(tmp(a), pp.at[p, j], tout.at[j - 2]).start()
        for j in (2, 3):
            pltpu.make_async_copy(tmp(2 * j - 4), pp.at[p, j], tout.at[j - 2]).wait()
            row_send(p, 3, j).start()

    def la_arrived(p, j):
        remote(la.at[p, j], la.at[p, j], fl.at[0, 0], lar.at[p, j], other).wait_recv()

    def lb_arrived(p, j):
        remote(lb.at[p, j], lb.at[p, j], fl.at[0, 0], lbr.at[p, j], other).wait_recv()

    def fin_copies(p, kk):
        row = 2 * p + core
        for t in range(2):
            yield (remote(fin.at[kk, t], rdst[2 + t].at[row], fsend.at[kk, t], rrecv.at[2 + t, row], other),
                   pltpu.make_async_copy(fin.at[kk, t], rdst[2 + t].at[row], fsend.at[kk, t]))

    def fin_wait(p, kk):
        for far, near in fin_copies(p, kk):
            @pl.when(core == kk)
            def _():
                near.wait()

            @pl.when(core != kk)
            def _():
                far.wait_send()

    def finish(p, kk, g):
        @pl.when(p > 0)
        def _():
            fin_wait(p - 1, kk)

        fin[kk, 0] = (g[:HD] * SCALE).T.astype(BF16)
        fin[kk, 1] = g[HD:].T.astype(BF16)
        for far, near in fin_copies(p, kk):
            @pl.when(core == kk)
            def _():
                near.start()

            @pl.when(core != kk)
            def _():
                far.start()

    def task_row(task):
        p = task // 2
        row = 2 * p + lax.rem(1 - core + lax.rem(task, 2), 2)
        i = 2 * chip + lax.rem(core + lax.rem(p, 2), 2)
        return row, i

    def kv_slot(t, slot, blk):
        return bufs[t].at[slot, pl.ds(pl.multiple_of(blk * BLK, BLK), BLK), :]

    def fetch(task):
        p = task // 2
        slot = lax.rem(task, 2)
        row, i = task_row(task)

        @pl.when(slot == 0)
        def _():
            @pl.loop(0, chip + 1)
            def _(cs):
                kv_arrived(p, 2 * cs + 1 - core)

            @pl.when(i != me)
            def _():
                for cp in swap_send(p // 2):
                    cp.wait_recv()

        @pl.loop(0, 2 * chip + 2)
        def _(blk):
            @pl.when(blk == me)
            def _():
                for t in range(2):
                    pltpu.make_async_copy(src[t].at[row], kv_slot(t, slot, blk), load.at[t, blk]).start()

            @pl.when(blk != me)
            def _():
                for t in range(2):
                    pltpu.make_async_copy(ndst[t].at[row, blk], kv_slot(t, slot, blk), load.at[t, blk]).start()

        @pl.when(i == me)
        def _():
            for t in (2, 3):
                pltpu.make_async_copy(src[t].at[row], bufs[t].at[slot], load.at[t, 0]).start()

        @pl.when(i != me)
        def _():
            for t in (2, 3):
                pltpu.make_async_copy(sdst[t - 2].at[2 * (p // 2) + lax.rem(row, 2)], bufs[t].at[slot],
                                      load.at[t, 0]).start()

    def fetch_wait(task):
        slot = lax.rem(task, 2)

        @pl.loop(0, 2 * chip + 2)
        def _(blk):
            for t in range(2):
                pltpu.make_async_copy(ndst[t].at[0, blk], kv_slot(t, slot, blk), load.at[t, blk]).wait()

        for t in (2, 3):
            pltpu.make_async_copy(src[t].at[0], bufs[t].at[slot], load.at[t, 0]).wait()

    fetch(0)

    @pl.loop(0, NA)
    def _(task):
        p = task // 2
        slot = lax.rem(task, 2)
        oslot = lax.rem(task, NSLOT)
        row, i = task_row(task)

        @pl.when((task + 2 < NP) & (lax.rem(chip, 2) == 1))
        def _():
            own_kv(task + 2, start)

        for c in (2, 3):
            @pl.when((chip == c) & (slot == 1) & (p + 1 < NP))
            def _():
                forward(p + 1, c)

        for when, rows in enumerate(LATER):
            @pl.when(task == when)
            def _():
                for hi in rows:
                    home_out(hi, start)

        fetch_wait(task)

        @pl.when((slot == 0) & (p > 0))
        def _():
            rows_leave(p - 1)

        @pl.when(task >= NSLOT)
        def _():
            row0, i0 = task_row(task - NSLOT)
            reply_wait(0, row0, i0, oslot)
            reply_wait(1, row0, i0, oslot)

        def after_forward():
            reply_start(0, row, i, oslot)

        def before_pass_c():
            @pl.when((chip == 1) & (task + 1 < NP))
            def _():
                forward(task + 1, 1)

            @pl.when(task + 1 < NA)
            def _():
                fetch(task + 1)

            @pl.when(slot == 0)
            def _():
                @pl.when(p > 0)
                def _():
                    @pl.loop(0, 2 * chip + 2)
                    def _(j):
                        pair_out(p - 1, j).wait_send()

                acc[0] = jnp.zeros((2 * HD, SEQ), F32)

            @pl.when(slot == 1)
            def _():
                @pl.loop(0, 2 * chip + 2)
                def _(j):
                    pair_out(p, j).wait_recv()
                    pltpu.make_async_copy(l1.at[p, j], piece(1, j), accin.at[j]).start()

                @pl.loop(0, 2 * chip + 2)
                def _(j):
                    pltpu.make_async_copy(l1.at[p, j], piece(1, j), accin.at[j]).wait()

        attn_tile(i, slot, oslot, slot, qb, dob, kb, vb, ob, dqb, S, acc, slot, oacc, mx, lx, qT, doT,
                  after_forward, before_pass_c)
        reply_start(1, row, i, oslot)

        @pl.when(slot == 0)
        def _():
            @pl.loop(0, 2 * chip + 2)
            def _(j):
                pair_out(p, j).start()

        @pl.when((slot == 0) & (p > 0) & (chip == 3))
        def _():
            join_chip2(p - 1)

        @pl.when(slot == 1)
        def _():
            for c in range(4):
                @on_chip(c)
                def _():
                    for j in kept(c):
                        row_keep(p, j).start()
                    if c == 3:
                        for kk in range(2):
                            finish(p, kk, acc[1, :, pl.ds((6 + kk) * BLK, BLK)])

    @pl.loop(NA - NSLOT, NA)
    def _(task):
        row0, i0 = task_row(task)
        reply_wait(0, row0, i0, lax.rem(task, NSLOT))
        reply_wait(1, row0, i0, lax.rem(task, NSLOT))

    @pl.loop(0, 2 * chip + 2)
    def _(j):
        pair_out(NP - 1, j).wait_send()

    rows_leave(NP - 1)

    @on_chip(3)
    def _():
        join_chip2(NP - 1)

    def pick(values):
        got = jnp.int32(values[0])
        for d in range(1, NDEV):
            got = jnp.where(me == d, values[d], got)
        return got

    hcount = pick([HOMES.count(d) for d in range(NDEV)])
    first = pick([HOMES.index(d) if d in HOMES else 0 for d in range(NDEV)])

    def home_block(step):
        return lax.rem(2 * chip - 1 - step + NDEV, NDEV)

    def home_row(h):
        return NA + first + h

    def home_arrived(t, h, i):
        view = hdst[t].at[h, i]
        remote(view, view, hsend.at[t, 0], hrecv.at[t, h, i], other).wait_recv()

    def home_kv(h):
        row = home_row(h)
        for t in range(2):
            pltpu.make_async_copy(src[t].at[row], kv_slot(t, h, me), load.at[t, me]).start()

        @pl.loop(1, NDEV)
        def _(step):
            i = partner(step)
            for t in range(2):
                home_arrived(t, h, i)
                pltpu.make_async_copy(hdst[t].at[h, i], kv_slot(t, h, i), load.at[t, i]).start()

        @pl.loop(0, NDEV)
        def _(i):
            for t in range(2):
                pltpu.make_async_copy(hdst[t].at[h, i], kv_slot(t, h, i), load.at[t, i]).wait()

    def home_fetch(task):
        h = task // NDEV
        step = lax.rem(task, NDEV)
        slot = lax.rem(task, 2)
        i = home_block(step)

        @pl.when(i == me)
        def _():
            for t in (2, 3):
                pltpu.make_async_copy(src[t].at[home_row(h)], bufs[t].at[slot], load.at[t, 0]).start()

        @pl.when(i != me)
        def _():
            for t in (2, 3):
                home_arrived(t, h, i)
                pltpu.make_async_copy(hdst[t].at[h, i], bufs[t].at[slot], load.at[t, 0]).start()

    def home_task(task):
        return home_row(task // NDEV), home_block(lax.rem(task, NDEV))

    stage = (os_, dqs)
    sstage = (dks, dvs)

    def put_down(t, task):
        row, i = home_task(task)
        idx = lax.rem(task, NSLOT)
        return (pltpu.make_async_copy(rbuf[t].at[idx], rdst[t].at[row], lout.at[t, idx]),
                pltpu.make_async_copy(rbuf[t].at[idx], stage[t].at[task], lout.at[t, idx]))

    def put_down_start(t, task):
        own, put = put_down(t, task)
        i = home_task(task)[1]

        @pl.when(i == me)
        def _():
            own.start()

        @pl.when(i != me)
        def _():
            put.start()

    def away(t, task):
        row, i = home_task(task)
        return remote(stage[t].at[task], rdst[t].at[row], asend.at[t, task], rrecv.at[t, row], i)

    def send_away(t, task):
        own, put = put_down(t, task)
        i = home_task(task)[1]

        @pl.when(i == me)
        def _():
            own.wait()

        @pl.when(i != me)
        def _():
            put.wait()
            away(t, task).start()

    def sum_down(t, h, j, away_too):
        target = sstage[t - 2].at[h, j] if away_too else rdst[t].at[home_row(h)]
        return pltpu.make_async_copy(rbuf[t], target, lout.at[t, 0])

    def sum_away(t, h, j):
        row = home_row(h)
        return remote(sstage[t - 2].at[h, j], rdst[t].at[row], ssend.at[t - 2, h, j], rrecv.at[t, row], j)

    @pl.when(hcount > 0)
    def _():
        home_fetch(0)

    @pl.loop(0, NDEV * hcount)
    def _(task):
        h = task // NDEV
        step = lax.rem(task, NDEV)
        slot = lax.rem(task, 2)
        oslot = lax.rem(task, NSLOT)
        row, i = home_task(task)

        @pl.when(step == 0)
        def _():
            home_kv(h)
            acc[h] = jnp.zeros((2 * HD, SEQ), F32)

        for t in (2, 3):
            pltpu.make_async_copy(src[t].at[0], bufs[t].at[slot], load.at[t, 0]).wait()

        @pl.when(task > 0)
        def _():
            send_away(1, task - 1)

        def after_forward():
            put_down_start(0, task)

        def before_pass_c():
            @pl.when(task + 1 < NDEV * hcount)
            def _():
                home_fetch(task + 1)

        attn_tile(i, slot, oslot, h, qb, dob, kb, vb, ob, dqb, S, acc, h, oacc, mx, lx, qT, doT,
                  after_forward, before_pass_c)
        put_down_start(1, task)
        send_away(0, task)

        def flush(j):
            o = pl.ds(pl.multiple_of(j * BLK, BLK), BLK)
            kst[...] = (acc[h, pl.ds(0, HD), o] * SCALE).T.astype(BF16)
            vst[...] = acc[h, pl.ds(HD, HD), o].T.astype(BF16)
            for where, away_too in ((j == me, False), (j != me, True)):
                @pl.when(where)
                def _():
                    for t in (2, 3):
                        sum_down(t, h, j, away_too).start()
                    for t in (2, 3):
                        sum_down(t, h, j, away_too).wait()
                        if away_too:
                            sum_away(t, h, j).start()

        @pl.when(step >= 2 * chip)
        def _():
            flush(i)

        @pl.when(step == NDEV - 1)
        def _():
            @pl.loop(0, 2 * chip)
            def _(j):
                flush(j)

    @pl.when(hcount > 0)
    def _():
        send_away(1, NDEV * hcount - 1)

    @pl.loop(0, NP)
    def _(p):
        @on_chip(1)
        def _():
            def join(j):
                la_arrived(p, j)
                take(pp.at[p, j], 0).start()
                take(la.at[p, j], 1).start()
                take(pp.at[p, j], 0).wait()
                take(la.at[p, j], 1).wait()

            for j in range(2):
                onward = lambda pq: remote(tmp(2 + j), la.at[pq, j], tout.at[j], lar.at[pq, j], plane(0))

                @pl.when((p > 0) & (p <= NP - LAST))
                def _():
                    onward(p - 1).wait_send()

                @pl.when(p < NP - LAST)
                def _():
                    join(j)
                    tmp(2 + j)[...] = tmp(0)[...] + tmp(1)[...]
                    onward(p).start()

            for j in (2, 3):
                join(j)
                finish(p, j - 2, tmp(0)[...] + tmp(1)[...])

        @on_chip(2)
        def _():
            for j in range(2):
                la_arrived(p, j)
                take(pp.at[p, 4 + j], 2 * j).start()
                take(la.at[p, j], 2 * j + 1).start()
                take(pp.at[p, 4 + j], 2 * j).wait()
                take(la.at[p, j], 2 * j + 1).wait()
                finish(p, j, tmp(2 * j)[...] + tmp(2 * j + 1)[...])

        @on_chip(0)
        def _():
            for j in range(2):
                la_arrived(p, j)
                lb_arrived(p, j)
                take(pp.at[p, j], 0).start()
                take(la.at[p, j], 1).start()
                take(lb.at[p, j], 2).start()
                take(pp.at[p, j], 0).wait()
                take(la.at[p, j], 1).wait()
                take(lb.at[p, j], 2).wait()

                @pl.when(p >= NP - LAST)
                def _():
                    came_by = lc.at[p - (NP - LAST), j]
                    remote(came_by, came_by, fl.at[0, 0], lcr.at[p - (NP - LAST), j], other).wait_recv()
                    take(came_by, 3).start()
                    take(came_by, 3).wait()
                    tmp(2)[...] += tmp(3)[...]

                finish(p, j, tmp(0)[...] + tmp(1)[...] + tmp(2)[...])

    for kk in range(2):
        fin_wait(NP - 1, kk)

    finished = lambda cp: cp.wait_send()

    @pl.loop(0, NP)
    def _(p):
        own_kv(p, finished)
        rows_left(p)
        for c in (1, 2, 3):
            @on_chip(c)
            def _():
                forward_done(p, c)

    @pl.loop(0, NDEV * hcount)
    def _(task):
        @pl.when(home_task(task)[1] != me)
        def _():
            away(0, task).wait_send()
            away(1, task).wait_send()
            for t in (2, 3):
                sum_away(t, task // NDEV, home_task(task)[1]).wait_send()

    for g in range(NP // 2):
        for cp in swap_send(g):
            cp.wait_send()
    for hi in range(len(HOMES)):
        home_out(hi, finished)

    def came(t, row):
        source = rbuf[t].at[0] if t < 2 else rbuf[t]
        remote(source, rdst[t].at[row], rsend.at[t, 0], rrecv.at[t, row], other).wait_recv()

    for hi in range(len(HOMES)):
        @pl.when(me != HOMES[hi])
        def _():
            for t in range(4):
                came(t, NA + hi)

    @pl.loop(0, NA)
    def _(row):
        @pl.when(lax.rem(row // 2, 2) == 1)
        def _():
            came(0, row)
            came(1, row)

        @pl.when(lax.rem(row, 2) != core)
        def _():
            came(2, row)
            came(3, row)


def solution(mesh):
    spec = P('data', ('ctxo', 'ctx'), None, None)
    any_spec = pl.BlockSpec(memory_space=pl.ANY)

    def local_attn(q_in, k_in, v_in, do_in):
        rows = q_in.shape[0]
        wide = (QR, HD)
        narrow = (BLK, HD)
        shape = lambda lead, tail, dtype=BF16: jax.ShapeDtypeStruct(lead + tail, dtype)
        pair = (2 * HD, BLK)
        vmem = pltpu.VMEM
        dma = pltpu.SemaphoreType.DMA
        call = pl.pallas_call(
            kernel,
            out_shape=[
                shape((rows,), wide), shape((rows,), wide), shape((rows,), narrow), shape((rows,), narrow),
                shape((2, NDEV), wide), shape((2, NDEV), wide), shape((2, NDEV), narrow), shape((2, NDEV), narrow),
                shape((NA, NDEV), narrow), shape((NA, NDEV), narrow), shape((NP,), wide), shape((NP,), wide),
                shape((2 * NDEV,), wide), shape((2 * NDEV,), wide),
                shape((2, NDEV), narrow), shape((2, NDEV), narrow),
                shape((NP, NDEV), pair, F32), shape((NP, 4), pair, F32), shape((NP, 2), pair, F32), shape((LAST, 2), pair, F32),
                shape((NP, 6), pair, F32),
            ],
            in_specs=[any_spec] * 4,
            out_specs=[any_spec] * 21,
            scratch_shapes=[
                vmem((2,) + wide, BF16), vmem((2,) + wide, BF16),
                vmem((2, SEQ, HD), BF16), vmem((2, SEQ, HD), BF16),
                vmem((NSLOT,) + wide, BF16), vmem((NSLOT,) + wide, BF16),
                vmem((BLK, HD), BF16), vmem((BLK, HD), BF16),
                vmem((2, 2) + narrow, BF16),
                vmem((QR, SEQ), F32), vmem((2, 2 * HD, SEQ), F32),
                vmem((QR, HD), F32),
                vmem((QR, 128), F32), vmem((QR, 128), F32),
                vmem((HD, QR), BF16), vmem((HD, QR), BF16),
                dma((2, NP, 4, 3)), dma((2, NP, NDEV)), dma((2, NP // 2)), dma((2, NP // 2)),
                dma((4, len(HOMES))), dma((4, 2, NDEV)), dma((2, NSLOT)), dma((4, rows)), dma((4, NDEV)), dma((4, NSLOT)),
                dma((NP, NDEV)), dma((NP, 4)), dma((NP, 2)), dma((LAST, 2)), dma((2, NDEV)), dma((NDEV,)), dma((2, 2)),
                dma((4,)), dma((2,)), dma((NP, 6)), dma((2, 2 * NDEV)), dma((2, 2, NDEV)),
            ],
            compiler_params=pltpu.CompilerParams(
                collective_id=0, has_side_effects=True, vmem_limit_bytes=67043328),
        )
        res = call(q_in.reshape((rows,) + wide), do_in.reshape((rows,) + wide),
                   k_in.reshape((rows,) + narrow), v_in.reshape((rows,) + narrow))
        return (res[0].reshape(q_in.shape), res[1].reshape(q_in.shape),
                res[2].reshape(k_in.shape), res[3].reshape(v_in.shape))

    return jax.shard_map(local_attn, mesh=mesh, in_specs=(spec,) * 4, out_specs=(spec,) * 4, check_vma=False)
```

```python
import functools
import math

import jax
import jax.numpy as jnp
from jax import lax
from jax.experimental import pallas as pl
from jax.experimental.pallas import tpu as pltpu
from jax.sharding import PartitionSpec as P

MESH = pl.DeviceIdType.MESH
NT = (((1,), (1,)), ((), ()))
F32 = jnp.float32
BF16 = jnp.bfloat16
NDEV = 8
BLK = 512
QR = 4 * BLK
HD = 128
SEQ = NDEV * BLK
SCALE = 1.0 / math.sqrt(HD)
SCALE2 = SCALE * math.log2(math.e)
DIAG = 256
RA = 1024
RB = 1024
RC = 1024
NSLOT = 2
NA = 10
NP = NA // 2
LAST = 2
DIRECT = 5
HOMES = (0, 0, 1, 2, 4, 5)
HSLOT = (0, 1, 0, 0, 0, 0)
EARLY = (0, 3, 2)
LATER = ((), (), (), (1,), (4, 5))


def lane_fold(op, s):
    acc = s[:, 0:128]
    for g in range(1, s.shape[1] // 128):
        acc = op(acc, s[:, g * 128:(g + 1) * 128])
    return acc


def lanes(x, width):
    return jnp.tile(x, (1, width // 128))


def attn_tile(blk, slot, oslot, kv, qb, dob, kb, vb, ob, dqb, S, acc, aslot, oacc, mx, lx, qT, doT, after_forward, before_pass_c):
    own = pl.multiple_of(blk * BLK, BLK)
    blocks = lambda n: [(r, n) for r in range(0, QR, n)]

    def diag(fn):
        for u in reversed(range(BLK // DIAG)):
            fn(u, DIAG * (u + 1), u * DIAG * 4, DIAG * 4)

    def sweep(chunk):
        @pl.loop(0, blk // 2)
        def _(j):
            chunk(pl.multiple_of(2 * j * BLK, BLK))
            chunk(pl.multiple_of((2 * j + 1) * BLK, BLK))

        @pl.when(lax.rem(blk, 2) == 1)
        def _():
            chunk(pl.multiple_of((blk - 1) * BLK, BLK))

    def score_diag(u, w, r, n):
        rs = pl.ds(r, n)
        s = lax.dot_general(qb[slot, rs, :], kb[kv, pl.ds(own, w), :], NT, preferred_element_type=F32)
        row = lax.broadcasted_iota(jnp.int32, (n, DIAG), 0) // 4
        col = lax.broadcasted_iota(jnp.int32, (n, DIAG), 1)
        sd = jnp.where(row >= col, s[:, w - DIAG:], -1e30)
        S[rs, pl.ds(own + (w - DIAG), DIAG)] = sd
        m = lane_fold(jnp.maximum, sd)
        if w > DIAG:
            S[rs, pl.ds(own, w - DIAG)] = s[:, :w - DIAG]
            m = jnp.maximum(m, lane_fold(jnp.maximum, s[:, :w - DIAG]))
        mx[rs, :] = m

    diag(score_diag)
    qT[...] = qb[slot].T
    doT[...] = dob[slot].T

    def chunk_a(o):
        for r, n in blocks(RA):
            rs = pl.ds(r, n)
            s = lax.dot_general(qb[slot, rs, :], kb[kv, pl.ds(o, BLK), :], NT, preferred_element_type=F32)
            S[rs, pl.ds(o, BLK)] = s
            mx[rs, :] = jnp.maximum(mx[rs, :], lane_fold(jnp.maximum, s))

    sweep(chunk_a)

    mx[...] = jnp.broadcast_to(jnp.max(mx[...], axis=1, keepdims=True) * SCALE2, (QR, 128))

    def probs(o, w, r, n, first):
        rs = pl.ds(r, n)
        p = jnp.exp2(S[rs, pl.ds(o, w)] * SCALE2 - lanes(mx[rs, :], w))
        S[rs, pl.ds(o, w)] = p
        ls = lane_fold(jnp.add, p)
        oo = jnp.dot(p.astype(BF16), vb[kv, pl.ds(o, w), :], preferred_element_type=F32)
        if first:
            lx[rs, :] = ls
            oacc[rs, :] = oo
        else:
            lx[rs, :] += ls
            oacc[rs, :] += oo

    diag(lambda u, w, r, n: probs(own, w, r, n, True))

    def chunk_b(o):
        for r, n in blocks(RB):
            probs(o, BLK, r, n, False)

    sweep(chunk_b)

    before_pass_c()
    lx[...] = jnp.broadcast_to(1.0 / jnp.sum(lx[...], axis=1, keepdims=True), (QR, 128))
    out = oacc[...] * lx[...]
    ob[oslot] = out.astype(BF16)
    mx[...] = jnp.broadcast_to(jnp.sum(out * dob[slot].astype(F32), axis=1, keepdims=True), (QR, 128))

    def grads(o, w, r, n, late):
        rs = pl.ds(r, n)

        def upstream():
            return lax.dot_general(dob[slot, rs, :], vb[kv, pl.ds(o, w), :], NT, preferred_element_type=F32)

        if late:
            pn = S[rs, pl.ds(o, w)] * lanes(lx[rs, :], w)
            dp = upstream()
        else:
            dp = upstream()
            pn = S[rs, pl.ds(o, w)] * lanes(lx[rs, :], w)
        ds = (pn * (dp - lanes(mx[rs, :], w))).astype(BF16)
        if late:
            gq = jnp.dot(ds, kb[kv, pl.ds(o, w), :], preferred_element_type=F32)
            gk = jnp.dot(qT[:, rs], ds, preferred_element_type=F32)
            gv = jnp.dot(doT[:, rs], pn.astype(BF16), preferred_element_type=F32)
        else:
            gv = jnp.dot(doT[:, rs], pn.astype(BF16), preferred_element_type=F32)
            gk = jnp.dot(qT[:, rs], ds, preferred_element_type=F32)
            gq = jnp.dot(ds, kb[kv, pl.ds(o, w), :], preferred_element_type=F32)
        return gv, gk, gq

    def grads_diag(u, w, r, n):
        gv, gk, gq = grads(own, w, r, n, False)
        oacc[pl.ds(r, n), :] = gq
        acc[aslot, pl.ds(HD, HD), pl.ds(own, w)] += gv
        acc[aslot, pl.ds(0, HD), pl.ds(own, w)] += gk

    diag(grads_diag)
    after_forward()

    @pl.loop(0, blk)
    def _(j):
        o = pl.multiple_of(j * BLK, BLK)
        av, ak = None, None
        for r, n in blocks(RC):
            gv, gk, gq = grads(o, BLK, r, n, True)
            oacc[pl.ds(r, n), :] += gq
            av = gv if av is None else av + gv
            ak = gk if ak is None else ak + gk
        acc[aslot, pl.ds(HD, HD), pl.ds(o, BLK)] += av
        acc[aslot, pl.ds(0, HD), pl.ds(o, BLK)] += ak

    dqb[oslot] = (oacc[...] * SCALE).astype(BF16)


def kernel(q, do, k, v, out, dq, dk, dv, qh, doh, kh, vh, kn, vn, qs, dos, os_, dqs, dks, dvs, l1, la, lb, lc, pp,
           qb, dob, kb, vb, ob, dqb, kst, vst, fin, S, acc, oacc, mx, lx, qT, doT,
           kvsend, kvrecv, swsend, swrecv, hsend, hrecv, rsend, rrecv, load, lout,
           l1r, lar, lbr, lcr, fl, accin, fsend, tin, tout, osend, asend, ssend):
    y = lax.axis_index('ctxo')
    b = lax.axis_index('ctx')
    x = b // 2
    core = lax.rem(b, 2)
    me = y * 4 + b
    chip = 2 * y + x
    other = 2 * chip + 1 - core

    def device(d):
        return (0, d // 4, lax.rem(d, 4))

    def plane(c):
        return 2 * c + core

    def on_chip(c):
        return pl.when(chip == c)

    def partner(step):
        off = lax.rem(2 * step, NDEV) + step // 4
        return (lax.rem(y + off // 4, 2) * 4 + lax.rem(x + lax.rem(off // 2, 2), 2) * 2
                + lax.rem(core + lax.rem(off, 2), 2))

    def remote(source, target, ssem, rsem, dev):
        return pltpu.make_async_remote_copy(src_ref=source, dst_ref=target, send_sem=ssem, recv_sem=rsem,
                                            device_id=device(dev), device_id_type=MESH)

    barrier = pltpu.get_barrier_semaphore()
    for step in range(1, NDEV):
        pl.semaphore_signal(barrier, inc=1, device_id=device(partner(step)), device_id_type=MESH)
    pl.semaphore_wait(barrier, NDEV - 1)

    src = (k, v, q, do)
    hdst = (kh, vh, qh, doh)
    ndst = (kn, vn)
    sdst = (qs, dos)
    bufs = (kb, vb, qb, dob)

    def kv_send(p, blk, kind, dev, own):
        for t in range(2):
            rows = pl.ds(2 * p, 2)
            source = src[t].at[rows] if own else ndst[t].at[rows, blk]
            yield remote(source, ndst[t].at[rows, blk], kvsend.at[t, p, blk // 2, kind], kvrecv.at[t, p, blk], dev)

    def kv_arrived(p, blk):
        for t in range(2):
            view = ndst[t].at[pl.ds(2 * p, 2), blk]
            remote(view, view, kvsend.at[t, p, 0, 0], kvrecv.at[t, p, blk], other).wait_recv()

    def own_kv(p, what):
        for c, targets in ((0, ((1, 0), (2, 2))), (1, ((3, 0),)), (2, ((3, 0),))):
            @on_chip(c)
            def _():
                for cc, kind in targets:
                    for cp in kv_send(p, me, kind, plane(cc), True):
                        what(cp)
        @pl.when((chip == 1) & (p < DIRECT))
        def _():
            for cp in kv_send(p, me, 2, plane(2), True):
                what(cp)

        for cp in kv_send(p, me, 1, other, True):
            what(cp)

    PASS = {1: ((0, 3),), 2: ((0, None), (1, None)), 3: ((1, 2), (2, None), (0, None))}

    def forward(p, c):
        for cs, relay in PASS[c]:
            blk = plane(cs)
            kv_arrived(p, blk)
            if relay is not None:
                @pl.when((p >= DIRECT) | (c == 1))
                def _():
                    for cp in kv_send(p, blk, 0, plane(relay), False):
                        cp.start()

            for cp in kv_send(p, blk, 1, other, False):
                cp.start()

    def forward_done(p, c):
        for cs, relay in PASS[c]:
            blk = plane(cs)
            if relay is not None:
                @pl.when((p >= DIRECT) | (c == 1))
                def _():
                    for cp in kv_send(p, blk, 0, plane(relay), False):
                        cp.wait_send()

            for cp in kv_send(p, blk, 1, other, False):
                cp.wait_send()

    def swap_send(g):
        for t in range(2):
            yield remote(src[2 + t].at[pl.ds(4 * g + 2, 2)], sdst[t].at[pl.ds(2 * g, 2)],
                         swsend.at[t, g], swrecv.at[t, g], other)

    def home_send(hi):
        for t in range(4):
            yield remote(src[t].at[NA + hi], hdst[t].at[HSLOT[hi], me], hsend.at[t, hi], hrecv.at[t, HSLOT[hi], me],
                         HOMES[hi])

    def home_out(hi, what):
        @pl.when(me != HOMES[hi])
        def _():
            for cp in home_send(hi):
                what(cp)

    start = lambda cp: cp.start()
    own_kv(0, start)

    @pl.when(lax.rem(chip, 2) == 0)
    def _():
        @pl.loop(1, NP)
        def _(p):
            own_kv(p, start)

    home_out(EARLY[0], start)
    for c in (1, 2, 3):
        @on_chip(c)
        def _():
            forward(0, c)

    @pl.when(lax.rem(chip, 2) == 1)
    def _():
        own_kv(1, start)

    for g in range(NP // 2):
        for cp in swap_send(g):
            cp.start()
    for hi in EARLY[1:]:
        home_out(hi, start)

    rbuf = (ob, dqb, kst, vst)
    rdst = (out, dq, dk, dv)

    def reply(t, row, i, idx):
        source = rbuf[t].at[idx]
        far = remote(source, rdst[t].at[row], rsend.at[t, idx], rrecv.at[t, row], i)
        near = pltpu.make_async_copy(source, rdst[t].at[row], lout.at[t, idx])
        return far, near

    def reply_start(t, row, i, idx):
        far, near = reply(t, row, i, idx)

        @pl.when(i == me)
        def _():
            near.start()

        @pl.when(i != me)
        def _():
            far.start()

    def reply_wait(t, row, i, idx):
        far, near = reply(t, row, i, idx)

        @pl.when(i == me)
        def _():
            near.wait()

        @pl.when(i != me)
        def _():
            far.wait_send()

    def tmp(idx):
        return S.at[pl.ds(2 * HD * idx, 2 * HD), pl.ds(0, BLK)]

    def take(source, idx):
        return pltpu.make_async_copy(source, tmp(idx), tin.at[idx])

    def piece(aslot, j):
        return acc.at[aslot, :, pl.ds(pl.multiple_of(j * BLK, BLK), BLK)]

    def pair_out(p, j):
        return remote(piece(0, j), l1.at[p, j], fl.at[0, j], l1r.at[p, j], other)

    def row_keep(p, j):
        return pltpu.make_async_copy(piece(1, j), pp.at[p, j], fl.at[1, j])

    def kept(c):
        return range(6 if c == 3 else 2 * c + 2)

    def row_send(p, c, j):
        target = {3: {0: (la, 0, lar, 1), 1: (la, 1, lar, 1), 2: (la, 2, lar, 1), 3: (la, 3, lar, 1),
                      4: (la, 0, lar, 2), 5: (la, 1, lar, 2)},
                  2: {0: (lb, 0, lbr, 0), 1: (lb, 1, lbr, 0), 2: (la, 0, lar, 3), 3: (la, 1, lar, 3)}}[c]
        land, idx, sem, cc = target[j]
        return remote(pp.at[p, j], land.at[p, idx], osend.at[p, j], sem.at[p, idx], plane(cc))

    SENT = {3: (4, 5, 0, 1), 2: (2, 3, 0, 1)}

    def rows_leave(p):
        for c in range(4):
            @on_chip(c)
            def _():
                for j in kept(c):
                    row_keep(p, j).wait()
                for j in SENT.get(c, ()):
                    if c == 3 and j < 2:
                        @pl.when(p < NP - LAST)
                        def _():
                            row_send(p, c, j).start()

                        @pl.when(p >= NP - LAST)
                        def _():
                            last_direct(p, j).start()
                    else:
                        row_send(p, c, j).start()
                if c == 1:
                    @pl.when(p >= NP - LAST)
                    def _():
                        for j in range(2):
                            last_onward(p, j).start()

    def last_direct(p, j):
        return remote(pp.at[p, j], lc.at[p - (NP - LAST), j], osend.at[p, j], lcr.at[p - (NP - LAST), j], plane(0))

    def last_onward(p, j):
        return remote(pp.at[p, j], la.at[p, j], osend.at[p, j], lar.at[p, j], plane(0))

    def rows_left(p):
        for c, js in ((3, range(6)), (2, range(4))):
            @on_chip(c)
            def _():
                for j in js:
                    row_send(p, c, j).wait_send()

        @pl.when((chip == 1) & (p >= NP - LAST))
        def _():
            for j in range(2):
                last_onward(p, j).wait_send()

    def join_chip2(p):
        for j in (2, 3):
            la_arrived(p, j - 2)
            take(pp.at[p, j], 2 * j - 4).start()
            take(la.at[p, j - 2], 2 * j - 3).start()
        for j in (2, 3):
            a, b = 2 * j - 4, 2 * j - 3
            take(pp.at[p, j], a).wait()
            take(la.at[p, j - 2], b).wait()
            tmp(a)[...] += tmp(b)[...]
            pltpu.make_async_copy(tmp(a), pp.at[p, j], tout.at[j - 2]).start()
        for j in (2, 3):
            pltpu.make_async_copy(tmp(2 * j - 4), pp.at[p, j], tout.at[j - 2]).wait()
            row_send(p, 3, j).start()

    def la_arrived(p, j):
        remote(la.at[p, j], la.at[p, j], fl.at[0, 0], lar.at[p, j], other).wait_recv()

    def lb_arrived(p, j):
        remote(lb.at[p, j], lb.at[p, j], fl.at[0, 0], lbr.at[p, j], other).wait_recv()

    def fin_copies(p, kk):
        row = 2 * p + core
        for t in range(2):
            yield (remote(fin.at[kk, t], rdst[2 + t].at[row], fsend.at[kk, t], rrecv.at[2 + t, row], other),
                   pltpu.make_async_copy(fin.at[kk, t], rdst[2 + t].at[row], fsend.at[kk, t]))

    def fin_wait(p, kk):
        for far, near in fin_copies(p, kk):
            @pl.when(core == kk)
            def _():
                near.wait()

            @pl.when(core != kk)
            def _():
                far.wait_send()

    def finish(p, kk, g):
        @pl.when(p > 0)
        def _():
            fin_wait(p - 1, kk)

        fin[kk, 0] = (g[:HD] * SCALE).T.astype(BF16)
        fin[kk, 1] = g[HD:].T.astype(BF16)
        for far, near in fin_copies(p, kk):
            @pl.when(core == kk)
            def _():
                near.start()

            @pl.when(core != kk)
            def _():
                far.start()

    def task_row(task):
        p = task // 2
        row = 2 * p + lax.rem(1 - core + lax.rem(task, 2), 2)
        i = 2 * chip + lax.rem(core + lax.rem(p, 2), 2)
        return row, i

    def kv_slot(t, slot, blk):
        return bufs[t].at[slot, pl.ds(pl.multiple_of(blk * BLK, BLK), BLK), :]

    def fetch(task):
        p = task // 2
        slot = lax.rem(task, 2)
        row, i = task_row(task)

        @pl.when(slot == 0)
        def _():
            @pl.loop(0, chip + 1)
            def _(cs):
                kv_arrived(p, 2 * cs + 1 - core)

            @pl.when(i != me)
            def _():
                for cp in swap_send(p // 2):
                    cp.wait_recv()

        @pl.loop(0, 2 * chip + 2)
        def _(blk):
            @pl.when(blk == me)
            def _():
                for t in range(2):
                    pltpu.make_async_copy(src[t].at[row], kv_slot(t, slot, blk), load.at[t, blk]).start()

            @pl.when(blk != me)
            def _():
                for t in range(2):
                    pltpu.make_async_copy(ndst[t].at[row, blk], kv_slot(t, slot, blk), load.at[t, blk]).start()

        @pl.when(i == me)
        def _():
            for t in (2, 3):
                pltpu.make_async_copy(src[t].at[row], bufs[t].at[slot], load.at[t, 0]).start()

        @pl.when(i != me)
        def _():
            for t in (2, 3):
                pltpu.make_async_copy(sdst[t - 2].at[2 * (p // 2) + lax.rem(row, 2)], bufs[t].at[slot],
                                      load.at[t, 0]).start()

    def fetch_wait(task):
        slot = lax.rem(task, 2)

        @pl.loop(0, 2 * chip + 2)
        def _(blk):
            for t in range(2):
                pltpu.make_async_copy(ndst[t].at[0, blk], kv_slot(t, slot, blk), load.at[t, blk]).wait()

        for t in (2, 3):
            pltpu.make_async_copy(src[t].at[0], bufs[t].at[slot], load.at[t, 0]).wait()

    fetch(0)

    @pl.loop(0, NA)
    def _(task):
        p = task // 2
        slot = lax.rem(task, 2)
        oslot = lax.rem(task, NSLOT)
        row, i = task_row(task)

        @pl.when((task + 2 < NP) & (lax.rem(chip, 2) == 1))
        def _():
            own_kv(task + 2, start)

        for c in (2, 3):
            @pl.when((chip == c) & (slot == 1) & (p + 1 < NP))
            def _():
                forward(p + 1, c)

        for when, rows in enumerate(LATER):
            @pl.when(task == when)
            def _():
                for hi in rows:
                    home_out(hi, start)

        fetch_wait(task)

        @pl.when((slot == 0) & (p > 0) & (chip == 3))
        def _():
            rows_leave(p - 1)

        @pl.when(task >= NSLOT)
        def _():
            row0, i0 = task_row(task - NSLOT)
            reply_wait(0, row0, i0, oslot)
            reply_wait(1, row0, i0, oslot)

        def after_forward():
            reply_start(0, row, i, oslot)

        def before_pass_c():
            @pl.when((chip == 1) & (task + 1 < NP))
            def _():
                forward(task + 1, 1)

            @pl.when(task + 1 < NA)
            def _():
                fetch(task + 1)

            @pl.when(slot == 0)
            def _():
                @pl.when(p > 0)
                def _():
                    @pl.loop(0, 2 * chip + 2)
                    def _(j):
                        pair_out(p - 1, j).wait_send()

                    @pl.when(chip < 3)
                    def _():
                        rows_leave(p - 1)

                acc[0] = jnp.zeros((2 * HD, SEQ), F32)

            @pl.when(slot == 1)
            def _():
                @pl.loop(0, 2 * chip + 2)
                def _(j):
                    pair_out(p, j).wait_recv()
                    pltpu.make_async_copy(l1.at[p, j], piece(1, j), accin.at[j]).start()

                @pl.loop(0, 2 * chip + 2)
                def _(j):
                    pltpu.make_async_copy(l1.at[p, j], piece(1, j), accin.at[j]).wait()

        attn_tile(i, slot, oslot, slot, qb, dob, kb, vb, ob, dqb, S, acc, slot, oacc, mx, lx, qT, doT,
                  after_forward, before_pass_c)
        reply_start(1, row, i, oslot)

        @pl.when(slot == 0)
        def _():
            @pl.loop(0, 2 * chip + 2)
            def _(j):
                pair_out(p, j).start()

        @pl.when((slot == 0) & (p > 0) & (chip == 3))
        def _():
            join_chip2(p - 1)

        @pl.when(slot == 1)
        def _():
            for c in range(4):
                @on_chip(c)
                def _():
                    for j in kept(c):
                        row_keep(p, j).start()
                    if c == 3:
                        for kk in range(2):
                            finish(p, kk, acc[1, :, pl.ds((6 + kk) * BLK, BLK)])

    @pl.loop(NA - NSLOT, NA)
    def _(task):
        row0, i0 = task_row(task)
        reply_wait(0, row0, i0, lax.rem(task, NSLOT))
        reply_wait(1, row0, i0, lax.rem(task, NSLOT))

    @pl.loop(0, 2 * chip + 2)
    def _(j):
        pair_out(NP - 1, j).wait_send()

    rows_leave(NP - 1)

    @on_chip(3)
    def _():
        join_chip2(NP - 1)

    def pick(values):
        got = jnp.int32(values[0])
        for d in range(1, NDEV):
            got = jnp.where(me == d, values[d], got)
        return got

    hcount = pick([HOMES.count(d) for d in range(NDEV)])
    first = pick([HOMES.index(d) if d in HOMES else 0 for d in range(NDEV)])

    def home_block(step):
        return lax.rem(2 * chip - 1 - step + NDEV, NDEV)

    def home_row(h):
        return NA + first + h

    def home_arrived(t, h, i):
        view = hdst[t].at[h, i]
        remote(view, view, hsend.at[t, 0], hrecv.at[t, h, i], other).wait_recv()

    def home_kv(h):
        row = home_row(h)
        for t in range(2):
            pltpu.make_async_copy(src[t].at[row], kv_slot(t, h, me), load.at[t, me]).start()

        @pl.loop(1, NDEV)
        def _(step):
            i = partner(step)
            for t in range(2):
                home_arrived(t, h, i)
                pltpu.make_async_copy(hdst[t].at[h, i], kv_slot(t, h, i), load.at[t, i]).start()

        @pl.loop(0, NDEV)
        def _(i):
            for t in range(2):
                pltpu.make_async_copy(hdst[t].at[h, i], kv_slot(t, h, i), load.at[t, i]).wait()

    def home_fetch(task):
        h = task // NDEV
        step = lax.rem(task, NDEV)
        slot = lax.rem(task, 2)
        i = home_block(step)

        @pl.when(i == me)
        def _():
            for t in (2, 3):
                pltpu.make_async_copy(src[t].at[home_row(h)], bufs[t].at[slot], load.at[t, 0]).start()

        @pl.when(i != me)
        def _():
            for t in (2, 3):
                home_arrived(t, h, i)
                pltpu.make_async_copy(hdst[t].at[h, i], bufs[t].at[slot], load.at[t, 0]).start()

    def home_task(task):
        return home_row(task // NDEV), home_block(lax.rem(task, NDEV))

    stage = (os_, dqs)
    sstage = (dks, dvs)

    def put_down(t, task):
        row, i = home_task(task)
        idx = lax.rem(task, NSLOT)
        return (pltpu.make_async_copy(rbuf[t].at[idx], rdst[t].at[row], lout.at[t, idx]),
                pltpu.make_async_copy(rbuf[t].at[idx], stage[t].at[task], lout.at[t, idx]))

    def put_down_start(t, task):
        own, put = put_down(t, task)
        i = home_task(task)[1]

        @pl.when(i == me)
        def _():
            own.start()

        @pl.when(i != me)
        def _():
            put.start()

    def away(t, task):
        row, i = home_task(task)
        return remote(stage[t].at[task], rdst[t].at[row], asend.at[t, task], rrecv.at[t, row], i)

    def send_away(t, task):
        own, put = put_down(t, task)
        i = home_task(task)[1]

        @pl.when(i == me)
        def _():
            own.wait()

        @pl.when(i != me)
        def _():
            put.wait()
            away(t, task).start()

    def sum_down(t, h, j, away_too):
        target = sstage[t - 2].at[h, j] if away_too else rdst[t].at[home_row(h)]
        return pltpu.make_async_copy(rbuf[t].at[lax.rem(j, 2)], target, lout.at[t, lax.rem(j, 2)])

    def sum_away(t, h, j):
        row = home_row(h)
        return remote(sstage[t - 2].at[h, j], rdst[t].at[row], ssend.at[t - 2, h, j], rrecv.at[t, row], j)

    @pl.when(hcount > 0)
    def _():
        home_fetch(0)

    @pl.loop(0, NDEV * hcount)
    def _(task):
        h = task // NDEV
        step = lax.rem(task, NDEV)
        slot = lax.rem(task, 2)
        oslot = lax.rem(task, NSLOT)
        row, i = home_task(task)

        @pl.when(step == 0)
        def _():
            home_kv(h)
            acc[h] = jnp.zeros((2 * HD, SEQ), F32)

        for t in (2, 3):
            pltpu.make_async_copy(src[t].at[0], bufs[t].at[slot], load.at[t, 0]).wait()

        @pl.when(task > 0)
        def _():
            send_away(1, task - 1)

        def after_forward():
            put_down_start(0, task)

        def before_pass_c():
            @pl.when(task + 1 < NDEV * hcount)
            def _():
                home_fetch(task + 1)

        attn_tile(i, slot, oslot, h, qb, dob, kb, vb, ob, dqb, S, acc, h, oacc, mx, lx, qT, doT,
                  after_forward, before_pass_c)
        put_down_start(1, task)
        send_away(0, task)

        def convert(j):
            o = pl.ds(pl.multiple_of(j * BLK, BLK), BLK)
            kst[lax.rem(j, 2)] = (acc[h, pl.ds(0, HD), o] * SCALE).T.astype(BF16)
            vst[lax.rem(j, 2)] = acc[h, pl.ds(HD, HD), o].T.astype(BF16)

        def down(j, away_too, what):
            for t in (2, 3):
                what(sum_down(t, h, j, away_too))

        def leave(j):
            down(j, True, lambda cp: cp.wait())
            for t in (2, 3):
                sum_away(t, h, j).start()

        @pl.when(step >= 2 * chip)
        def _():
            convert(i)

            @pl.when(i == me)
            def _():
                down(i, False, start)
                down(i, False, lambda cp: cp.wait())

            @pl.when(i != me)
            def _():
                down(i, True, start)
                leave(i)

        @pl.when(step == NDEV - 1)
        def _():
            @pl.loop(0, 2 * chip)
            def _(j):
                convert(j)
                down(j, True, start)

                @pl.when(j > 0)
                def _():
                    leave(j - 1)

            @pl.when(chip > 0)
            def _():
                leave(2 * chip - 1)

    @pl.when(hcount > 0)
    def _():
        send_away(1, NDEV * hcount - 1)

    @pl.loop(0, NP)
    def _(p):
        @on_chip(1)
        def _():
            def join(j):
                la_arrived(p, j)
                take(pp.at[p, j], 0).start()
                take(la.at[p, j], 1).start()
                take(pp.at[p, j], 0).wait()
                take(la.at[p, j], 1).wait()

            for j in range(2):
                onward = lambda pq: remote(tmp(2 + j), la.at[pq, j], tout.at[j], lar.at[pq, j], plane(0))

                @pl.when((p > 0) & (p <= NP - LAST))
                def _():
                    onward(p - 1).wait_send()

                @pl.when(p < NP - LAST)
                def _():
                    join(j)
                    tmp(2 + j)[...] = tmp(0)[...] + tmp(1)[...]
                    onward(p).start()

            for j in (2, 3):
                join(j)
                finish(p, j - 2, tmp(0)[...] + tmp(1)[...])

        @on_chip(2)
        def _():
            for j in range(2):
                la_arrived(p, j)
                take(pp.at[p, 4 + j], 2 * j).start()
                take(la.at[p, j], 2 * j + 1).start()
                take(pp.at[p, 4 + j], 2 * j).wait()
                take(la.at[p, j], 2 * j + 1).wait()
                finish(p, j, tmp(2 * j)[...] + tmp(2 * j + 1)[...])

        @on_chip(0)
        def _():
            for j in range(2):
                la_arrived(p, j)
                lb_arrived(p, j)
                take(pp.at[p, j], 0).start()
                take(la.at[p, j], 1).start()
                take(lb.at[p, j], 2).start()
                take(pp.at[p, j], 0).wait()
                take(la.at[p, j], 1).wait()
                take(lb.at[p, j], 2).wait()

                @pl.when(p >= NP - LAST)
                def _():
                    came_by = lc.at[p - (NP - LAST), j]
                    remote(came_by, came_by, fl.at[0, 0], lcr.at[p - (NP - LAST), j], other).wait_recv()
                    take(came_by, 3).start()
                    take(came_by, 3).wait()
                    tmp(2)[...] += tmp(3)[...]

                finish(p, j, tmp(0)[...] + tmp(1)[...] + tmp(2)[...])

    for kk in range(2):
        fin_wait(NP - 1, kk)

    finished = lambda cp: cp.wait_send()

    @pl.loop(0, NP)
    def _(p):
        own_kv(p, finished)
        rows_left(p)
        for c in (1, 2, 3):
            @on_chip(c)
            def _():
                forward_done(p, c)

    @pl.loop(0, NDEV * hcount)
    def _(task):
        @pl.when(home_task(task)[1] != me)
        def _():
            away(0, task).wait_send()
            away(1, task).wait_send()
            for t in (2, 3):
                sum_away(t, task // NDEV, home_task(task)[1]).wait_send()

    for g in range(NP // 2):
        for cp in swap_send(g):
            cp.wait_send()
    for hi in range(len(HOMES)):
        home_out(hi, finished)

    def came(t, row):
        source = rbuf[t].at[0]
        remote(source, rdst[t].at[row], rsend.at[t, 0], rrecv.at[t, row], other).wait_recv()

    for hi in range(len(HOMES)):
        @pl.when(me != HOMES[hi])
        def _():
            for t in range(4):
                came(t, NA + hi)

    @pl.loop(0, NA)
    def _(row):
        @pl.when(lax.rem(row // 2, 2) == 1)
        def _():
            came(0, row)
            came(1, row)

        @pl.when(lax.rem(row, 2) != core)
        def _():
            came(2, row)
            came(3, row)


def solution(mesh):
    spec = P('data', ('ctxo', 'ctx'), None, None)
    any_spec = pl.BlockSpec(memory_space=pl.ANY)

    def local_attn(q_in, k_in, v_in, do_in):
        rows = q_in.shape[0]
        wide = (QR, HD)
        narrow = (BLK, HD)
        shape = lambda lead, tail, dtype=BF16: jax.ShapeDtypeStruct(lead + tail, dtype)
        pair = (2 * HD, BLK)
        vmem = pltpu.VMEM
        dma = pltpu.SemaphoreType.DMA
        call = pl.pallas_call(
            kernel,
            out_shape=[
                shape((rows,), wide), shape((rows,), wide), shape((rows,), narrow), shape((rows,), narrow),
                shape((2, NDEV), wide), shape((2, NDEV), wide), shape((2, NDEV), narrow), shape((2, NDEV), narrow),
                shape((NA, NDEV), narrow), shape((NA, NDEV), narrow), shape((NP,), wide), shape((NP,), wide),
                shape((2 * NDEV,), wide), shape((2 * NDEV,), wide),
                shape((2, NDEV), narrow), shape((2, NDEV), narrow),
                shape((NP, NDEV), pair, F32), shape((NP, 4), pair, F32), shape((NP, 2), pair, F32), shape((LAST, 2), pair, F32),
                shape((NP, 6), pair, F32),
            ],
            in_specs=[any_spec] * 4,
            out_specs=[any_spec] * 21,
            scratch_shapes=[
                vmem((2,) + wide, BF16), vmem((2,) + wide, BF16),
                vmem((2, SEQ, HD), BF16), vmem((2, SEQ, HD), BF16),
                vmem((NSLOT,) + wide, BF16), vmem((NSLOT,) + wide, BF16),
                vmem((2, BLK, HD), BF16), vmem((2, BLK, HD), BF16),
                vmem((2, 2) + narrow, BF16),
                vmem((QR, SEQ), F32), vmem((2, 2 * HD, SEQ), F32),
                vmem((QR, HD), F32),
                vmem((QR, 128), F32), vmem((QR, 128), F32),
                vmem((HD, QR), BF16), vmem((HD, QR), BF16),
                dma((2, NP, 4, 3)), dma((2, NP, NDEV)), dma((2, NP // 2)), dma((2, NP // 2)),
                dma((4, len(HOMES))), dma((4, 2, NDEV)), dma((2, NSLOT)), dma((4, rows)), dma((4, NDEV)), dma((4, NSLOT)),
                dma((NP, NDEV)), dma((NP, 4)), dma((NP, 2)), dma((LAST, 2)), dma((2, NDEV)), dma((NDEV,)), dma((2, 2)),
                dma((4,)), dma((2,)), dma((NP, 6)), dma((2, 2 * NDEV)), dma((2, 2, NDEV)),
            ],
            compiler_params=pltpu.CompilerParams(
                collective_id=0, has_side_effects=True, vmem_limit_bytes=67043328),
        )
        res = call(q_in.reshape((rows,) + wide), do_in.reshape((rows,) + wide),
                   k_in.reshape((rows,) + narrow), v_in.reshape((rows,) + narrow))
        return (res[0].reshape(q_in.shape), res[1].reshape(q_in.shape),
                res[2].reshape(k_in.shape), res[3].reshape(v_in.shape))

    return jax.shard_map(local_attn, mesh=mesh, in_specs=(spec,) * 4, out_specs=(spec,) * 4, check_vma=False)
```

```python
import functools
import math

import jax
import jax.numpy as jnp
from jax import lax
from jax.experimental import pallas as pl
from jax.experimental.pallas import tpu as pltpu
from jax.sharding import PartitionSpec as P

MESH = pl.DeviceIdType.MESH
NT = (((1,), (1,)), ((), ()))
F32 = jnp.float32
BF16 = jnp.bfloat16
NDEV = 8
BLK = 512
QR = 4 * BLK
HD = 128
SEQ = NDEV * BLK
SCALE = 1.0 / math.sqrt(HD)
SCALE2 = SCALE * math.log2(math.e)
DIAG = 256
RA = 1024
RB = 1024
RC = 1024
NSLOT = 2
NA = 10
NP = NA // 2
LAST = 1
DIRECT = 5
HOMES = (0, 0, 1, 2, 4, 5)
HSLOT = (0, 1, 0, 0, 0, 0)
EARLY = (0, 3, 2)
LATER = ((), (), (), (1,), (4, 5))


def lane_fold(op, s):
    acc = s[:, 0:128]
    for g in range(1, s.shape[1] // 128):
        acc = op(acc, s[:, g * 128:(g + 1) * 128])
    return acc


def lanes(x, width):
    return jnp.tile(x, (1, width // 128))


def attn_tile(blk, slot, oslot, kv, qb, dob, kb, vb, ob, dqb, S, acc, aslot, oacc, mx, lx, qT, doT, after_forward, before_pass_c):
    own = pl.multiple_of(blk * BLK, BLK)
    blocks = lambda n: [(r, n) for r in range(0, QR, n)]

    def diag(fn):
        for u in reversed(range(BLK // DIAG)):
            fn(u, DIAG * (u + 1), u * DIAG * 4, DIAG * 4)

    def sweep(chunk):
        @pl.loop(0, blk // 2)
        def _(j):
            chunk(pl.multiple_of(2 * j * BLK, BLK))
            chunk(pl.multiple_of((2 * j + 1) * BLK, BLK))

        @pl.when(lax.rem(blk, 2) == 1)
        def _():
            chunk(pl.multiple_of((blk - 1) * BLK, BLK))

    def score_diag(u, w, r, n):
        rs = pl.ds(r, n)
        s = lax.dot_general(qb[slot, rs, :], kb[kv, pl.ds(own, w), :], NT, preferred_element_type=F32)
        row = lax.broadcasted_iota(jnp.int32, (n, DIAG), 0) // 4
        col = lax.broadcasted_iota(jnp.int32, (n, DIAG), 1)
        sd = jnp.where(row >= col, s[:, w - DIAG:], -1e30)
        S[rs, pl.ds(own + (w - DIAG), DIAG)] = sd
        m = lane_fold(jnp.maximum, sd)
        if w > DIAG:
            S[rs, pl.ds(own, w - DIAG)] = s[:, :w - DIAG]
            m = jnp.maximum(m, lane_fold(jnp.maximum, s[:, :w - DIAG]))
        mx[rs, :] = m

    diag(score_diag)
    qT[...] = qb[slot].T
    doT[...] = dob[slot].T

    def chunk_a(o):
        for r, n in blocks(RA):
            rs = pl.ds(r, n)
            s = lax.dot_general(qb[slot, rs, :], kb[kv, pl.ds(o, BLK), :], NT, preferred_element_type=F32)
            S[rs, pl.ds(o, BLK)] = s
            mx[rs, :] = jnp.maximum(mx[rs, :], lane_fold(jnp.maximum, s))

    sweep(chunk_a)

    mx[...] = jnp.broadcast_to(jnp.max(mx[...], axis=1, keepdims=True) * SCALE2, (QR, 128))

    def probs(o, w, r, n, first):
        rs = pl.ds(r, n)
        p = jnp.exp2(S[rs, pl.ds(o, w)] * SCALE2 - lanes(mx[rs, :], w))
        S[rs, pl.ds(o, w)] = p
        ls = lane_fold(jnp.add, p)
        oo = jnp.dot(p.astype(BF16), vb[kv, pl.ds(o, w), :], preferred_element_type=F32)
        if first:
            lx[rs, :] = ls
            oacc[rs, :] = oo
        else:
            lx[rs, :] += ls
            oacc[rs, :] += oo

    diag(lambda u, w, r, n: probs(own, w, r, n, True))

    def chunk_b(o):
        for r, n in blocks(RB):
            probs(o, BLK, r, n, False)

    sweep(chunk_b)

    before_pass_c()
    lx[...] = jnp.broadcast_to(1.0 / jnp.sum(lx[...], axis=1, keepdims=True), (QR, 128))
    out = oacc[...] * lx[...]
    ob[oslot] = out.astype(BF16)
    mx[...] = jnp.broadcast_to(jnp.sum(out * dob[slot].astype(F32), axis=1, keepdims=True), (QR, 128))

    def grads(o, w, r, n, late):
        rs = pl.ds(r, n)

        def upstream():
            return lax.dot_general(dob[slot, rs, :], vb[kv, pl.ds(o, w), :], NT, preferred_element_type=F32)

        if late:
            pn = S[rs, pl.ds(o, w)] * lanes(lx[rs, :], w)
            dp = upstream()
        else:
            dp = upstream()
            pn = S[rs, pl.ds(o, w)] * lanes(lx[rs, :], w)
        ds = (pn * (dp - lanes(mx[rs, :], w))).astype(BF16)
        if late:
            gq = jnp.dot(ds, kb[kv, pl.ds(o, w), :], preferred_element_type=F32)
            gk = jnp.dot(qT[:, rs], ds, preferred_element_type=F32)
            gv = jnp.dot(doT[:, rs], pn.astype(BF16), preferred_element_type=F32)
        else:
            gv = jnp.dot(doT[:, rs], pn.astype(BF16), preferred_element_type=F32)
            gk = jnp.dot(qT[:, rs], ds, preferred_element_type=F32)
            gq = jnp.dot(ds, kb[kv, pl.ds(o, w), :], preferred_element_type=F32)
        return gv, gk, gq

    def grads_diag(u, w, r, n):
        gv, gk, gq = grads(own, w, r, n, False)
        oacc[pl.ds(r, n), :] = gq
        acc[aslot, pl.ds(HD, HD), pl.ds(own, w)] += gv
        acc[aslot, pl.ds(0, HD), pl.ds(own, w)] += gk

    diag(grads_diag)
    after_forward()

    @pl.loop(0, blk)
    def _(j):
        o = pl.multiple_of(j * BLK, BLK)
        av, ak = None, None
        for r, n in blocks(RC):
            gv, gk, gq = grads(o, BLK, r, n, True)
            oacc[pl.ds(r, n), :] += gq
            av = gv if av is None else av + gv
            ak = gk if ak is None else ak + gk
        acc[aslot, pl.ds(HD, HD), pl.ds(o, BLK)] += av
        acc[aslot, pl.ds(0, HD), pl.ds(o, BLK)] += ak

    dqb[oslot] = (oacc[...] * SCALE).astype(BF16)


def kernel(q, do, k, v, out, dq, dk, dv, qh, doh, kh, vh, kn, vn, qs, dos, os_, dqs, dks, dvs, l1, la, lb, lc, pp,
           qb, dob, kb, vb, ob, dqb, kst, vst, fin, S, acc, oacc, mx, lx, qT, doT,
           kvsend, kvrecv, swsend, swrecv, hsend, hrecv, rsend, rrecv, load, lout,
           l1r, lar, lbr, lcr, fl, accin, fsend, tin, tout, osend, asend, ssend):
    y = lax.axis_index('ctxo')
    b = lax.axis_index('ctx')
    x = b // 2
    core = lax.rem(b, 2)
    me = y * 4 + b
    chip = 2 * y + x
    other = 2 * chip + 1 - core

    def device(d):
        return (0, d // 4, lax.rem(d, 4))

    def plane(c):
        return 2 * c + core

    def on_chip(c):
        return pl.when(chip == c)

    def partner(step):
        off = lax.rem(2 * step, NDEV) + step // 4
        return (lax.rem(y + off // 4, 2) * 4 + lax.rem(x + lax.rem(off // 2, 2), 2) * 2
                + lax.rem(core + lax.rem(off, 2), 2))

    def remote(source, target, ssem, rsem, dev):
        return pltpu.make_async_remote_copy(src_ref=source, dst_ref=target, send_sem=ssem, recv_sem=rsem,
                                            device_id=device(dev), device_id_type=MESH)

    barrier = pltpu.get_barrier_semaphore()
    for step in range(1, NDEV):
        pl.semaphore_signal(barrier, inc=1, device_id=device(partner(step)), device_id_type=MESH)
    pl.semaphore_wait(barrier, NDEV - 1)

    src = (k, v, q, do)
    hdst = (kh, vh, qh, doh)
    ndst = (kn, vn)
    sdst = (qs, dos)
    bufs = (kb, vb, qb, dob)

    def kv_send(p, blk, kind, dev, own):
        for t in range(2):
            rows = pl.ds(2 * p, 2)
            source = src[t].at[rows] if own else ndst[t].at[rows, blk]
            yield remote(source, ndst[t].at[rows, blk], kvsend.at[t, p, blk // 2, kind], kvrecv.at[t, p, blk], dev)

    def kv_arrived(p, blk):
        for t in range(2):
            view = ndst[t].at[pl.ds(2 * p, 2), blk]
            remote(view, view, kvsend.at[t, p, 0, 0], kvrecv.at[t, p, blk], other).wait_recv()

    def own_kv(p, what):
        for c, targets in ((0, ((1, 0), (2, 2))), (1, ((3, 0),)), (2, ((3, 0),))):
            @on_chip(c)
            def _():
                for cc, kind in targets:
                    for cp in kv_send(p, me, kind, plane(cc), True):
                        what(cp)
        @pl.when((chip == 1) & (p < DIRECT))
        def _():
            for cp in kv_send(p, me, 2, plane(2), True):
                what(cp)

        for cp in kv_send(p, me, 1, other, True):
            what(cp)

    PASS = {1: ((0, 3),), 2: ((0, None), (1, None)), 3: ((1, 2), (2, None), (0, None))}

    def forward(p, c):
        for cs, relay in PASS[c]:
            blk = plane(cs)
            kv_arrived(p, blk)
            if relay is not None:
                @pl.when((p >= DIRECT) | (c == 1))
                def _():
                    for cp in kv_send(p, blk, 0, plane(relay), False):
                        cp.start()

            for cp in kv_send(p, blk, 1, other, False):
                cp.start()

    def forward_done(p, c):
        for cs, relay in PASS[c]:
            blk = plane(cs)
            if relay is not None:
                @pl.when((p >= DIRECT) | (c == 1))
                def _():
                    for cp in kv_send(p, blk, 0, plane(relay), False):
                        cp.wait_send()

            for cp in kv_send(p, blk, 1, other, False):
                cp.wait_send()

    def swap_send(g):
        for t in range(2):
            yield remote(src[2 + t].at[pl.ds(4 * g + 2, 2)], sdst[t].at[pl.ds(2 * g, 2)],
                         swsend.at[t, g], swrecv.at[t, g], other)

    def home_send(hi):
        for t in range(4):
            yield remote(src[t].at[NA + hi], hdst[t].at[HSLOT[hi], me], hsend.at[t, hi], hrecv.at[t, HSLOT[hi], me],
                         HOMES[hi])

    def home_out(hi, what):
        @pl.when(me != HOMES[hi])
        def _():
            for cp in home_send(hi):
                what(cp)

    start = lambda cp: cp.start()
    own_kv(0, start)

    @pl.when(lax.rem(chip, 2) == 0)
    def _():
        @pl.loop(1, NP)
        def _(p):
            own_kv(p, start)

    home_out(EARLY[0], start)
    for c in (1, 2, 3):
        @on_chip(c)
        def _():
            forward(0, c)

    @pl.when(lax.rem(chip, 2) == 1)
    def _():
        own_kv(1, start)

    for g in range(NP // 2):
        for cp in swap_send(g):
            cp.start()
    for hi in EARLY[1:]:
        home_out(hi, start)

    rbuf = (ob, dqb, kst, vst)
    rdst = (out, dq, dk, dv)

    def reply(t, row, i, idx):
        source = rbuf[t].at[idx]
        far = remote(source, rdst[t].at[row], rsend.at[t, idx], rrecv.at[t, row], i)
        near = pltpu.make_async_copy(source, rdst[t].at[row], lout.at[t, idx])
        return far, near

    def reply_start(t, row, i, idx):
        far, near = reply(t, row, i, idx)

        @pl.when(i == me)
        def _():
            near.start()

        @pl.when(i != me)
        def _():
            far.start()

    def reply_wait(t, row, i, idx):
        far, near = reply(t, row, i, idx)

        @pl.when(i == me)
        def _():
            near.wait()

        @pl.when(i != me)
        def _():
            far.wait_send()

    def tmp(idx):
        return S.at[pl.ds(2 * HD * idx, 2 * HD), pl.ds(0, BLK)]

    def take(source, idx):
        return pltpu.make_async_copy(source, tmp(idx), tin.at[idx])

    def piece(aslot, j):
        return acc.at[aslot, :, pl.ds(pl.multiple_of(j * BLK, BLK), BLK)]

    def pair_out(p, j):
        return remote(piece(0, j), l1.at[p, j], fl.at[0, j], l1r.at[p, j], other)

    def row_keep(p, j):
        return pltpu.make_async_copy(piece(1, j), pp.at[p, j], fl.at[1, j])

    def kept(c):
        return range(6 if c == 3 else 2 * c + 2)

    def row_send(p, c, j):
        target = {3: {0: (la, 0, lar, 1), 1: (la, 1, lar, 1), 2: (la, 2, lar, 1), 3: (la, 3, lar, 1),
                      4: (la, 0, lar, 2), 5: (la, 1, lar, 2)},
                  2: {0: (lb, 0, lbr, 0), 1: (lb, 1, lbr, 0), 2: (la, 0, lar, 3), 3: (la, 1, lar, 3)}}[c]
        land, idx, sem, cc = target[j]
        return remote(pp.at[p, j], land.at[p, idx], osend.at[p, j], sem.at[p, idx], plane(cc))

    SENT = {3: (4, 5, 0, 1), 2: (2, 3, 0, 1)}

    def rows_leave(p):
        for c in range(4):
            @on_chip(c)
            def _():
                for j in kept(c):
                    row_keep(p, j).wait()
                for j in SENT.get(c, ()):
                    if c == 3 and j < 2:
                        @pl.when(p < NP - LAST)
                        def _():
                            row_send(p, c, j).start()

                        @pl.when(p >= NP - LAST)
                        def _():
                            last_direct(p, j).start()
                    else:
                        row_send(p, c, j).start()
                if c == 1:
                    @pl.when(p >= NP - LAST)
                    def _():
                        for j in range(2):
                            last_onward(p, j).start()

    def last_direct(p, j):
        return remote(pp.at[p, j], lc.at[p - (NP - LAST), j], osend.at[p, j], lcr.at[p - (NP - LAST), j], plane(0))

    def last_onward(p, j):
        return remote(pp.at[p, j], la.at[p, j], osend.at[p, j], lar.at[p, j], plane(0))

    def rows_left(p):
        for c, js in ((3, range(6)), (2, range(4))):
            @on_chip(c)
            def _():
                for j in js:
                    row_send(p, c, j).wait_send()

        @pl.when((chip == 1) & (p >= NP - LAST))
        def _():
            for j in range(2):
                last_onward(p, j).wait_send()

    def join_chip2(p):
        for j in (2, 3):
            la_arrived(p, j - 2)
            take(pp.at[p, j], 2 * j - 4).start()
            take(la.at[p, j - 2], 2 * j - 3).start()
        for j in (2, 3):
            a, b = 2 * j - 4, 2 * j - 3
            take(pp.at[p, j], a).wait()
            take(la.at[p, j - 2], b).wait()
            tmp(a)[...] += tmp(b)[...]
            pltpu.make_async_copy(tmp(a), pp.at[p, j], tout.at[j - 2]).start()
        for j in (2, 3):
            pltpu.make_async_copy(tmp(2 * j - 4), pp.at[p, j], tout.at[j - 2]).wait()
            row_send(p, 3, j).start()

    def la_arrived(p, j):
        remote(la.at[p, j], la.at[p, j], fl.at[0, 0], lar.at[p, j], other).wait_recv()

    def lb_arrived(p, j):
        remote(lb.at[p, j], lb.at[p, j], fl.at[0, 0], lbr.at[p, j], other).wait_recv()

    def fin_copies(p, kk):
        row = 2 * p + core
        for t in range(2):
            yield (remote(fin.at[kk, t], rdst[2 + t].at[row], fsend.at[kk, t], rrecv.at[2 + t, row], other),
                   pltpu.make_async_copy(fin.at[kk, t], rdst[2 + t].at[row], fsend.at[kk, t]))

    def fin_wait(p, kk):
        for far, near in fin_copies(p, kk):
            @pl.when(core == kk)
            def _():
                near.wait()

            @pl.when(core != kk)
            def _():
                far.wait_send()

    def finish(p, kk, g):
        @pl.when(p > 0)
        def _():
            fin_wait(p - 1, kk)

        fin[kk, 0] = (g[:HD] * SCALE).T.astype(BF16)
        fin[kk, 1] = g[HD:].T.astype(BF16)
        for far, near in fin_copies(p, kk):
            @pl.when(core == kk)
            def _():
                near.start()

            @pl.when(core != kk)
            def _():
                far.start()

    def task_row(task):
        p = task // 2
        row = 2 * p + lax.rem(1 - core + lax.rem(task, 2), 2)
        i = 2 * chip + lax.rem(core + lax.rem(p, 2), 2)
        return row, i

    def kv_slot(t, slot, blk):
        return bufs[t].at[slot, pl.ds(pl.multiple_of(blk * BLK, BLK), BLK), :]

    def fetch(task):
        p = task // 2
        slot = lax.rem(task, 2)
        row, i = task_row(task)

        @pl.when(slot == 0)
        def _():
            @pl.loop(0, chip + 1)
            def _(cs):
                kv_arrived(p, 2 * cs + 1 - core)

            @pl.when(i != me)
            def _():
                for cp in swap_send(p // 2):
                    cp.wait_recv()

        @pl.loop(0, 2 * chip + 2)
        def _(blk):
            @pl.when(blk == me)
            def _():
                for t in range(2):
                    pltpu.make_async_copy(src[t].at[row], kv_slot(t, slot, blk), load.at[t, blk]).start()

            @pl.when(blk != me)
            def _():
                for t in range(2):
                    pltpu.make_async_copy(ndst[t].at[row, blk], kv_slot(t, slot, blk), load.at[t, blk]).start()

        @pl.when(i == me)
        def _():
            for t in (2, 3):
                pltpu.make_async_copy(src[t].at[row], bufs[t].at[slot], load.at[t, 0]).start()

        @pl.when(i != me)
        def _():
            for t in (2, 3):
                pltpu.make_async_copy(sdst[t - 2].at[2 * (p // 2) + lax.rem(row, 2)], bufs[t].at[slot],
                                      load.at[t, 0]).start()

    def fetch_wait(task):
        slot = lax.rem(task, 2)

        @pl.loop(0, 2 * chip + 2)
        def _(blk):
            for t in range(2):
                pltpu.make_async_copy(ndst[t].at[0, blk], kv_slot(t, slot, blk), load.at[t, blk]).wait()

        for t in (2, 3):
            pltpu.make_async_copy(src[t].at[0], bufs[t].at[slot], load.at[t, 0]).wait()

    fetch(0)

    @pl.loop(0, NA)
    def _(task):
        p = task // 2
        slot = lax.rem(task, 2)
        oslot = lax.rem(task, NSLOT)
        row, i = task_row(task)

        @pl.when((task + 2 < NP) & (lax.rem(chip, 2) == 1))
        def _():
            own_kv(task + 2, start)

        for c in (2, 3):
            @pl.when((chip == c) & (slot == 1) & (p + 1 < NP))
            def _():
                forward(p + 1, c)

        for when, rows in enumerate(LATER):
            @pl.when(task == when)
            def _():
                for hi in rows:
                    home_out(hi, start)

        fetch_wait(task)

        @pl.when((slot == 0) & (p > 0) & (chip == 3))
        def _():
            rows_leave(p - 1)

        @pl.when(task >= NSLOT)
        def _():
            row0, i0 = task_row(task - NSLOT)
            reply_wait(0, row0, i0, oslot)
            reply_wait(1, row0, i0, oslot)

        def after_forward():
            reply_start(0, row, i, oslot)

        def before_pass_c():
            @pl.when((chip == 1) & (task + 1 < NP))
            def _():
                forward(task + 1, 1)

            @pl.when(task + 1 < NA)
            def _():
                fetch(task + 1)

            @pl.when(slot == 0)
            def _():
                @pl.when(p > 0)
                def _():
                    @pl.loop(0, 2 * chip + 2)
                    def _(j):
                        pair_out(p - 1, j).wait_send()

                    @pl.when(chip < 3)
                    def _():
                        rows_leave(p - 1)

                acc[0] = jnp.zeros((2 * HD, SEQ), F32)

            @pl.when(slot == 1)
            def _():
                @pl.loop(0, 2 * chip + 2)
                def _(j):
                    pair_out(p, j).wait_recv()
                    pltpu.make_async_copy(l1.at[p, j], piece(1, j), accin.at[j]).start()

                @pl.loop(0, 2 * chip + 2)
                def _(j):
                    pltpu.make_async_copy(l1.at[p, j], piece(1, j), accin.at[j]).wait()

        attn_tile(i, slot, oslot, slot, qb, dob, kb, vb, ob, dqb, S, acc, slot, oacc, mx, lx, qT, doT,
                  after_forward, before_pass_c)
        reply_start(1, row, i, oslot)

        @pl.when(slot == 0)
        def _():
            @pl.loop(0, 2 * chip + 2)
            def _(j):
                pair_out(p, j).start()

        @pl.when((slot == 0) & (p > 0) & (chip == 3))
        def _():
            join_chip2(p - 1)

        @pl.when(slot == 1)
        def _():
            for c in range(4):
                @on_chip(c)
                def _():
                    for j in kept(c):
                        row_keep(p, j).start()
                    if c == 3:
                        for kk in range(2):
                            finish(p, kk, acc[1, :, pl.ds((6 + kk) * BLK, BLK)])

    @pl.loop(NA - NSLOT, NA)
    def _(task):
        row0, i0 = task_row(task)
        reply_wait(0, row0, i0, lax.rem(task, NSLOT))
        reply_wait(1, row0, i0, lax.rem(task, NSLOT))

    @pl.loop(0, 2 * chip + 2)
    def _(j):
        pair_out(NP - 1, j).wait_send()

    rows_leave(NP - 1)

    @on_chip(3)
    def _():
        join_chip2(NP - 1)

    def pick(values):
        got = jnp.int32(values[0])
        for d in range(1, NDEV):
            got = jnp.where(me == d, values[d], got)
        return got

    hcount = pick([HOMES.count(d) for d in range(NDEV)])
    first = pick([HOMES.index(d) if d in HOMES else 0 for d in range(NDEV)])

    def home_block(step):
        return lax.rem(2 * chip - 1 - step + NDEV, NDEV)

    def home_row(h):
        return NA + first + h

    def home_arrived(t, h, i):
        view = hdst[t].at[h, i]
        remote(view, view, hsend.at[t, 0], hrecv.at[t, h, i], other).wait_recv()

    def home_kv(h):
        row = home_row(h)
        for t in range(2):
            pltpu.make_async_copy(src[t].at[row], kv_slot(t, h, me), load.at[t, me]).start()

        @pl.loop(1, NDEV)
        def _(step):
            i = partner(step)
            for t in range(2):
                home_arrived(t, h, i)
                pltpu.make_async_copy(hdst[t].at[h, i], kv_slot(t, h, i), load.at[t, i]).start()

        @pl.loop(0, NDEV)
        def _(i):
            for t in range(2):
                pltpu.make_async_copy(hdst[t].at[h, i], kv_slot(t, h, i), load.at[t, i]).wait()

    def home_fetch(task):
        h = task // NDEV
        step = lax.rem(task, NDEV)
        slot = lax.rem(task, 2)
        i = home_block(step)

        @pl.when(i == me)
        def _():
            for t in (2, 3):
                pltpu.make_async_copy(src[t].at[home_row(h)], bufs[t].at[slot], load.at[t, 0]).start()

        @pl.when(i != me)
        def _():
            for t in (2, 3):
                home_arrived(t, h, i)
                pltpu.make_async_copy(hdst[t].at[h, i], bufs[t].at[slot], load.at[t, 0]).start()

    def home_task(task):
        return home_row(task // NDEV), home_block(lax.rem(task, NDEV))

    stage = (os_, dqs)
    sstage = (dks, dvs)

    def put_down(t, task):
        row, i = home_task(task)
        idx = lax.rem(task, NSLOT)
        return (pltpu.make_async_copy(rbuf[t].at[idx], rdst[t].at[row], lout.at[t, idx]),
                pltpu.make_async_copy(rbuf[t].at[idx], stage[t].at[task], lout.at[t, idx]))

    def put_down_start(t, task):
        own, put = put_down(t, task)
        i = home_task(task)[1]

        @pl.when(i == me)
        def _():
            own.start()

        @pl.when(i != me)
        def _():
            put.start()

    def away(t, task):
        row, i = home_task(task)
        return remote(stage[t].at[task], rdst[t].at[row], asend.at[t, task], rrecv.at[t, row], i)

    def send_away(t, task):
        own, put = put_down(t, task)
        i = home_task(task)[1]

        @pl.when(i == me)
        def _():
            own.wait()

        @pl.when(i != me)
        def _():
            put.wait()
            away(t, task).start()

    def sum_down(t, h, j, away_too):
        target = sstage[t - 2].at[h, j] if away_too else rdst[t].at[home_row(h)]
        return pltpu.make_async_copy(rbuf[t].at[lax.rem(j, 2)], target, lout.at[t, lax.rem(j, 2)])

    def sum_away(t, h, j):
        row = home_row(h)
        return remote(sstage[t - 2].at[h, j], rdst[t].at[row], ssend.at[t - 2, h, j], rrecv.at[t, row], j)

    @pl.when(hcount > 0)
    def _():
        home_fetch(0)

    @pl.loop(0, NDEV * hcount)
    def _(task):
        h = task // NDEV
        step = lax.rem(task, NDEV)
        slot = lax.rem(task, 2)
        oslot = lax.rem(task, NSLOT)
        row, i = home_task(task)

        @pl.when(step == 0)
        def _():
            home_kv(h)
            acc[h] = jnp.zeros((2 * HD, SEQ), F32)

        for t in (2, 3):
            pltpu.make_async_copy(src[t].at[0], bufs[t].at[slot], load.at[t, 0]).wait()

        @pl.when(task > 0)
        def _():
            send_away(1, task - 1)

        def after_forward():
            put_down_start(0, task)

        def before_pass_c():
            @pl.when(task + 1 < NDEV * hcount)
            def _():
                home_fetch(task + 1)

        attn_tile(i, slot, oslot, h, qb, dob, kb, vb, ob, dqb, S, acc, h, oacc, mx, lx, qT, doT,
                  after_forward, before_pass_c)
        put_down_start(1, task)
        send_away(0, task)

        def convert(j):
            o = pl.ds(pl.multiple_of(j * BLK, BLK), BLK)
            kst[lax.rem(j, 2)] = (acc[h, pl.ds(0, HD), o] * SCALE).T.astype(BF16)
            vst[lax.rem(j, 2)] = acc[h, pl.ds(HD, HD), o].T.astype(BF16)

        def down(j, away_too, what):
            for t in (2, 3):
                what(sum_down(t, h, j, away_too))

        def leave(j):
            down(j, True, lambda cp: cp.wait())
            for t in (2, 3):
                sum_away(t, h, j).start()

        @pl.when(step >= 2 * chip)
        def _():
            convert(i)

            @pl.when(i == me)
            def _():
                down(i, False, start)
                down(i, False, lambda cp: cp.wait())

            @pl.when(i != me)
            def _():
                down(i, True, start)
                leave(i)

        @pl.when(step == NDEV - 1)
        def _():
            @pl.loop(0, 2 * chip)
            def _(j):
                convert(j)
                down(j, True, start)

                @pl.when(j > 0)
                def _():
                    leave(j - 1)

            @pl.when(chip > 0)
            def _():
                leave(2 * chip - 1)

    @pl.when(hcount > 0)
    def _():
        send_away(1, NDEV * hcount - 1)

    @pl.loop(0, NP)
    def _(p):
        @on_chip(1)
        def _():
            def join(j):
                la_arrived(p, j)
                take(pp.at[p, j], 0).start()
                take(la.at[p, j], 1).start()
                take(pp.at[p, j], 0).wait()
                take(la.at[p, j], 1).wait()

            for j in range(2):
                onward = lambda pq: remote(tmp(2 + j), la.at[pq, j], tout.at[j], lar.at[pq, j], plane(0))

                @pl.when((p > 0) & (p <= NP - LAST))
                def _():
                    onward(p - 1).wait_send()

                @pl.when(p < NP - LAST)
                def _():
                    join(j)
                    tmp(2 + j)[...] = tmp(0)[...] + tmp(1)[...]
                    onward(p).start()

            for j in (2, 3):
                join(j)
                finish(p, j - 2, tmp(0)[...] + tmp(1)[...])

        @on_chip(2)
        def _():
            for j in range(2):
                la_arrived(p, j)
                take(pp.at[p, 4 + j], 2 * j).start()
                take(la.at[p, j], 2 * j + 1).start()
                take(pp.at[p, 4 + j], 2 * j).wait()
                take(la.at[p, j], 2 * j + 1).wait()
                finish(p, j, tmp(2 * j)[...] + tmp(2 * j + 1)[...])

        @on_chip(0)
        def _():
            for j in range(2):
                la_arrived(p, j)
                lb_arrived(p, j)
                take(pp.at[p, j], 0).start()
                take(la.at[p, j], 1).start()
                take(lb.at[p, j], 2).start()
                take(pp.at[p, j], 0).wait()
                take(la.at[p, j], 1).wait()
                take(lb.at[p, j], 2).wait()

                @pl.when(p >= NP - LAST)
                def _():
                    came_by = lc.at[p - (NP - LAST), j]
                    remote(came_by, came_by, fl.at[0, 0], lcr.at[p - (NP - LAST), j], other).wait_recv()
                    take(came_by, 3).start()
                    take(came_by, 3).wait()
                    tmp(2)[...] += tmp(3)[...]

                finish(p, j, tmp(0)[...] + tmp(1)[...] + tmp(2)[...])

    for kk in range(2):
        fin_wait(NP - 1, kk)

    finished = lambda cp: cp.wait_send()

    @pl.loop(0, NP)
    def _(p):
        own_kv(p, finished)
        rows_left(p)
        for c in (1, 2, 3):
            @on_chip(c)
            def _():
                forward_done(p, c)

    @pl.loop(0, NDEV * hcount)
    def _(task):
        @pl.when(home_task(task)[1] != me)
        def _():
            away(0, task).wait_send()
            away(1, task).wait_send()
            for t in (2, 3):
                sum_away(t, task // NDEV, home_task(task)[1]).wait_send()

    for g in range(NP // 2):
        for cp in swap_send(g):
            cp.wait_send()
    for hi in range(len(HOMES)):
        home_out(hi, finished)

    def came(t, row):
        source = rbuf[t].at[0]
        remote(source, rdst[t].at[row], rsend.at[t, 0], rrecv.at[t, row], other).wait_recv()

    for hi in range(len(HOMES)):
        @pl.when(me != HOMES[hi])
        def _():
            for t in range(4):
                came(t, NA + hi)

    @pl.loop(0, NA)
    def _(row):
        @pl.when(lax.rem(row // 2, 2) == 1)
        def _():
            came(0, row)
            came(1, row)

        @pl.when(lax.rem(row, 2) != core)
        def _():
            came(2, row)
            came(3, row)


def solution(mesh):
    spec = P('data', ('ctxo', 'ctx'), None, None)
    any_spec = pl.BlockSpec(memory_space=pl.ANY)

    def local_attn(q_in, k_in, v_in, do_in):
        rows = q_in.shape[0]
        wide = (QR, HD)
        narrow = (BLK, HD)
        shape = lambda lead, tail, dtype=BF16: jax.ShapeDtypeStruct(lead + tail, dtype)
        pair = (2 * HD, BLK)
        vmem = pltpu.VMEM
        dma = pltpu.SemaphoreType.DMA
        call = pl.pallas_call(
            kernel,
            out_shape=[
                shape((rows,), wide), shape((rows,), wide), shape((rows,), narrow), shape((rows,), narrow),
                shape((2, NDEV), wide), shape((2, NDEV), wide), shape((2, NDEV), narrow), shape((2, NDEV), narrow),
                shape((NA, NDEV), narrow), shape((NA, NDEV), narrow), shape((NP,), wide), shape((NP,), wide),
                shape((2 * NDEV,), wide), shape((2 * NDEV,), wide),
                shape((2, NDEV), narrow), shape((2, NDEV), narrow),
                shape((NP, NDEV), pair, F32), shape((NP, 4), pair, F32), shape((NP, 2), pair, F32), shape((LAST, 2), pair, F32),
                shape((NP, 6), pair, F32),
            ],
            in_specs=[any_spec] * 4,
            out_specs=[any_spec] * 21,
            scratch_shapes=[
                vmem((2,) + wide, BF16), vmem((2,) + wide, BF16),
                vmem((2, SEQ, HD), BF16), vmem((2, SEQ, HD), BF16),
                vmem((NSLOT,) + wide, BF16), vmem((NSLOT,) + wide, BF16),
                vmem((2, BLK, HD), BF16), vmem((2, BLK, HD), BF16),
                vmem((2, 2) + narrow, BF16),
                vmem((QR, SEQ), F32), vmem((2, 2 * HD, SEQ), F32),
                vmem((QR, HD), F32),
                vmem((QR, 128), F32), vmem((QR, 128), F32),
                vmem((HD, QR), BF16), vmem((HD, QR), BF16),
                dma((2, NP, 4, 3)), dma((2, NP, NDEV)), dma((2, NP // 2)), dma((2, NP // 2)),
                dma((4, len(HOMES))), dma((4, 2, NDEV)), dma((2, NSLOT)), dma((4, rows)), dma((4, NDEV)), dma((4, NSLOT)),
                dma((NP, NDEV)), dma((NP, 4)), dma((NP, 2)), dma((LAST, 2)), dma((2, NDEV)), dma((NDEV,)), dma((2, 2)),
                dma((4,)), dma((2,)), dma((NP, 6)), dma((2, 2 * NDEV)), dma((2, 2, NDEV)),
            ],
            compiler_params=pltpu.CompilerParams(
                collective_id=0, has_side_effects=True, vmem_limit_bytes=67043328),
        )
        res = call(q_in.reshape((rows,) + wide), do_in.reshape((rows,) + wide),
                   k_in.reshape((rows,) + narrow), v_in.reshape((rows,) + narrow))
        return (res[0].reshape(q_in.shape), res[1].reshape(q_in.shape),
                res[2].reshape(k_in.shape), res[3].reshape(v_in.shape))

    return jax.shard_map(local_attn, mesh=mesh, in_specs=(spec,) * 4, out_specs=(spec,) * 4, check_vma=False)
```
